32 devices in a mesh: px: 4 (over y, x), py: 8 (over z, core).
Axes of the slice: x: 2, y: 2, z: 4, core: 2. Of those that a mesh axis runs over, the one named last changes fastest.
Arguments:
- base_cell: int32 [4, 8, 4096, 3], P('px', 'py'), may hold values from 0 to 255, as said below
- cell_offset: float32 [4, 8, 4096, 3], P('px', 'py'), may hold values from 0 to 1
- charges: float32 [4, 8, 4096], P('px', 'py'), may hold values from -4 to 4
- spacing: float32 [3], replicated, may hold values from 0.9 to 1.2
- ewald_beta: float32 [1], replicated, may hold values from 0.3 to 0.42
Outputs:
- forces: float32 [4, 8, 4096, 3], P('px', 'py')
- atom_energy: float32 [4, 8, 4096], P('px', 'py')
The draws below stay inside these ranges and needn't reach their ends.
Inputs may be any that keep to these rules, and one draw needn't show every extreme that they name: base_cell[i, j, a, 0] lies in [i * 16, (i + 1) * 16), base_cell[i, j, a, 1] in [j * 16, (j + 1) * 16), base_cell[i, j, a, 2] in [0, 256); within these ranges cells are uniform.
All inputs are finite; a program needn't handle non-finite values.
Results may differ from the reference program's by a relative error of at most 0.0003.
Values sent between devices are 32-bit elements.
A program may use at most 64 MiB of HBM per device.

```python
import jax
import jax.numpy as jnp

CX = 16
CY = 16
NZ = 256
ATOM_DEV = 4096
BX = 4
BY = 8
NX = 64
NY = 128


def draw_base_cell(key, part):
    first, second, third = jax.random.split(key, 3)
    shape_out = (BX, BY, ATOM_DEV)
    cell_x = jax.random.randint(first, shape_out, 0, CX, dtype=jnp.int32) + (jnp.arange(BX, dtype=jnp.int32) * CX)[:, None, None]
    cell_y = jax.random.randint(second, shape_out, 0, CY, dtype=jnp.int32) + (jnp.arange(BY, dtype=jnp.int32) * CY)[None, :, None]
    cell_z = jax.random.randint(third, shape_out, 0, NZ, dtype=jnp.int32)
    return jnp.stack([cell_x, cell_y, cell_z], axis=-1).astype(jnp.int32)


def levels(own_key, shape, cuts, smallest, largest):
    def one(dim, blocks):
        draws = jax.random.uniform(jax.random.fold_in(jax.random.fold_in(own_key, 6), dim), (blocks,), jnp.float32, smallest / len(cuts), largest / len(cuts))
        return jnp.repeat(jnp.exp(draws), shape[dim] // blocks).reshape((-1,) + (1,) * (len(shape) - dim - 1))

    factor_of = one(*cuts[0])
    for cut in cuts[1:]:
        factor_of = factor_of * one(*cut)
    return factor_of


def noise(stream_key, extent, spread, reach, shards=(), kind=jnp.bfloat16):
    loudness = levels(stream_key, extent, shards, -0.22, 0.18) if shards else 1.0
    entries = jax.random.normal(stream_key, extent, jnp.float32) * spread * loudness
    return jnp.minimum(jnp.maximum(entries, -reach), reach).astype(kind)


def setup_inputs(seed: int = 0) -> dict:
    arg_keys = jax.random.split(jax.random.key(seed), 6)
    return {
        "base_cell": draw_base_cell(jax.random.fold_in(arg_keys[5], 71), 0),
        "cell_offset": jnp.clip(1.0 * jax.random.uniform(arg_keys[1], (BX, BY, ATOM_DEV, 3), jnp.float32) ** levels(arg_keys[1], (BX, BY, ATOM_DEV, 3), ((0, 4), (1, 8)), -0.2, 0.2), 0.0, 1.0),
        "charges": noise(arg_keys[2], (BX, BY, ATOM_DEV), 1.0, 4.0, ((0, 4), (1, 8)), jnp.float32),
        "spacing": jnp.clip(jax.random.uniform(arg_keys[3], (3,), jnp.float32, 0.9, 1.2), 0.9, 1.2),
        "ewald_beta": jnp.clip(jax.random.uniform(arg_keys[4], (1,), jnp.float32, 0.3, 0.42), 0.3, 0.42),
    }


def spline_weights(offsets):
    square = offsets * offsets
    cube = square * offsets
    rest = 1.0 - offsets
    values = jnp.stack([rest * rest * rest / 6.0, (3.0 * cube - 6.0 * square + 4.0) / 6.0, (-3.0 * cube + 3.0 * square + 3.0 * offsets + 1.0) / 6.0, cube / 6.0], axis=-1)
    slopes = jnp.stack([-0.5 * rest * rest, 1.5 * square - 2.0 * offsets, -1.5 * square + offsets + 0.5, 0.5 * square], axis=-1)
    return values, slopes


def influence(starts, lengths, totals, spacing, screening):
    squares = jnp.zeros((1, 1, 1), jnp.float32)
    moduli = jnp.ones((1, 1, 1), jnp.float32)
    volume = spacing[0] * spacing[1] * spacing[2] * float(totals[0] * totals[1] * totals[2])
    for dimension in range(3):
        freq_index = starts[dimension] + jnp.arange(lengths[dimension], dtype=jnp.int32)
        signed = jnp.where(2 * freq_index < totals[dimension], freq_index, freq_index - totals[dimension]).astype(jnp.float32)
        frequency = signed / (spacing[dimension] * totals[dimension])
        cosine = jnp.cos((2.0 * jnp.pi / totals[dimension]) * freq_index.astype(jnp.float32))
        modulus = 1.0 / (((2.0 + cosine) / 3.0) ** 2)
        reshape_to = [1, 1, 1]
        reshape_to[dimension] = lengths[dimension]
        squares = squares + (frequency * frequency).reshape(reshape_to)
        moduli = moduli * modulus.reshape(reshape_to)
    safe_square = jnp.where(squares > 0.0, squares, 1.0)
    table = jnp.exp(-(jnp.pi ** 2) * safe_square / (screening * screening)) / (jnp.pi * volume * safe_square) * moduli
    return jnp.where(squares > 0.0, table, 0.0)


def reference(base_cell, cell_offset, charges, spacing, ewald_beta):
    cell_ids = base_cell.reshape(-1, 3)
    values, slopes = spline_weights(cell_offset.reshape(-1, 3))
    charge = charges.reshape(-1)
    totals = (NX, NY, NZ)
    stencil = [(shift_x, shift_y, shift_z) for shift_x in range(4) for shift_y in range(4) for shift_z in range(4)]

    def corners(offsets):
        return ((cell_ids[:, 0] + offsets[0]) % NX, (cell_ids[:, 1] + offsets[1]) % NY, (cell_ids[:, 2] + offsets[2]) % NZ)

    charge_grid = jnp.zeros(totals, jnp.float32)
    for offsets in stencil:
        weight = values[:, 0, offsets[0]] * values[:, 1, offsets[1]] * values[:, 2, offsets[2]]
        charge_grid = charge_grid.at[corners(offsets)].add(charge * weight)
    table = influence((0, 0, 0), totals, totals, spacing, ewald_beta[0])
    potential = jnp.real(jnp.fft.ifftn(table * jnp.fft.fftn(charge_grid), norm="forward"))
    sampled = jnp.zeros_like(charge)
    gradient_x = jnp.zeros_like(charge)
    gradient_y = jnp.zeros_like(charge)
    gradient_z = jnp.zeros_like(charge)
    for offsets in stencil:
        local_value = potential[corners(offsets)]
        value_x = values[:, 0, offsets[0]]
        value_y = values[:, 1, offsets[1]]
        value_z = values[:, 2, offsets[2]]
        sampled = sampled + local_value * value_x * value_y * value_z
        gradient_x = gradient_x + local_value * slopes[:, 0, offsets[0]] * value_y * value_z
        gradient_y = gradient_y + local_value * value_x * slopes[:, 1, offsets[1]] * value_z
        gradient_z = gradient_z + local_value * value_x * value_y * slopes[:, 2, offsets[2]]
    gradient = jnp.stack([gradient_x, gradient_y, gradient_z], axis=1)
    forces = -charge[:, None] * gradient / spacing[None, :]
    return forces.reshape(base_cell.shape), (0.5 * charge * sampled).reshape(charges.shape)
```

```python
import functools

import jax
import jax.numpy as jnp
import numpy as np
from jax import lax
from jax.experimental import pallas as pl
from jax.experimental.pallas import tpu as pltpu
from jax.sharding import PartitionSpec as P

CX = 16
CY = 16
NZ = 256
SPAN = CX + 3
RIM = 4
MAIN = SPAN * CY
ROWS = -(-(MAIN + SPAN * RIM) // 128) * 128
TILE = 512
VMEM_LIMIT = 60 * 1024 * 1024
NN = (((1,), (0,)), ((), ()))
NT = (((1,), (1,)), ((), ()))
TN = (((0,), (0,)), ((), ()))


def cas(positions, length):
    angles = 2.0 * np.pi / length * (np.outer(np.arange(length), positions) % length)
    return np.cos(angles) + np.sin(angles)


def halves(value):
    high = value.astype(jnp.bfloat16)
    return high, (value - high.astype(jnp.float32)).astype(jnp.bfloat16)


def constant_halves(table):
    table = np.asarray(table, np.float32)
    high = table.astype(jnp.bfloat16)
    return jnp.asarray(high), jnp.asarray((table - high.astype(np.float32)).astype(jnp.bfloat16))


def dot3(left, right, dims):
    def product(a, b):
        return lax.dot_general(a, b, dims, preferred_element_type=jnp.float32)

    return product(left[0], right[0]) + (product(left[0], right[1]) + product(left[1], right[0]))


def spline_values(t):
    rest = 1.0 - t
    square = t * t
    cube = square * t
    return (
        rest * rest * rest / 6.0,
        (3.0 * cube - 6.0 * square + 4.0) / 6.0,
        (-3.0 * cube + 3.0 * square + 3.0 * t + 1.0) / 6.0,
        cube / 6.0,
    )


def spline_slopes(t):
    rest = 1.0 - t
    square = t * t
    return (-0.5 * rest * rest, 1.5 * square - 2.0 * t, -1.5 * square + t + 0.5, 0.5 * square)


def pick(masks, weights):
    chosen = jnp.where(masks[3], weights[3], 0.0)
    for step in (2, 1, 0):
        chosen = jnp.where(masks[step], weights[step], chosen)
    return chosen


def masks_of(slots, start):
    steps = slots - start
    return [steps == step for step in range(4)]


def rows_iota(rows, width):
    return lax.broadcasted_iota(jnp.int32, (rows, width), 0)


class Stencil:
    def __init__(self, cells, offs, span):
        near_x = cells[0:1, span] - lax.axis_index("px") * CX
        near_y = cells[1:2, span] - lax.axis_index("py") * CY
        near_z = cells[2:3, span]
        width = near_x.shape[1]
        rim = rows_iota(ROWS - MAIN, width)
        self.x = masks_of(rows_iota(24, width), near_x)
        self.y = masks_of(rows_iota(CY, width), near_y)
        self.rim_x = masks_of(rim // RIM, near_x)
        self.rim_y = masks_of(CY + rim % RIM, near_y)
        steps = (rows_iota(NZ, width) - near_z) & (NZ - 1)
        self.z = [steps == step for step in range(4)]
        t = offs[:, span]
        self.values = [spline_values(t[d : d + 1]) for d in range(3)]
        self.slopes = [spline_slopes(t[d : d + 1]) for d in range(3)]


def spread_kernel(cells, offs, charge, tz_h, tz_l, out, grid):
    grid[...] = jnp.zeros_like(grid)

    @pl.loop(0, charge.shape[1] // TILE)
    def _(step):
        span = pl.ds(pl.multiple_of(step * TILE, TILE), TILE)
        near = Stencil(cells, offs, span)
        amount = charge[:, span]
        row_x = pick(near.x, [w * amount for w in near.values[0]])
        row_y = pick(near.y, near.values[1])
        rim = pick(near.rim_x, [w * amount for w in near.values[0]]) * pick(
            near.rim_y, near.values[1]
        )
        planes = jnp.concatenate([row_x[x : x + 1] * row_y for x in range(SPAN)] + [rim], axis=0)
        grid[...] += dot3(halves(planes), halves(pick(near.z, near.values[2])), NT)

    out[...] = dot3((tz_h[...], tz_l[...]), halves(grid[...]), NT)


def middle_kernel(
    pieces_x, pieces_y, got, spacing, beta, ty_h, ty_l, mx_h, mx_l, row1, row3, rowm, col2, colm,
    sent, turned, wide,
):
    slice_z = NZ // (pieces_x * pieces_y)
    chunk = pieces_x * slice_z
    total_x = CX * pieces_x
    total_y = CY * pieces_y

    def corners():
        for x in range(SPAN):
            for j in range(pieces_y):
                lanes = pl.ds(x * chunk, chunk)
                own = pl.ds(j * chunk, chunk)
                yield pl.ds(x * CY, CY), pl.ds(j * CY, CY), own, lanes
                yield pl.ds(MAIN + x * RIM, RIM), pl.ds(total_y + j * RIM, RIM), own, lanes

    turned[...] = got[...].T
    wide[...] = jnp.zeros_like(wide)
    for narrow_rows, wide_rows, own, lanes in corners():
        wide[wide_rows, lanes] = turned[narrow_rows, own]
    ty = (ty_h[...], ty_l[...])
    mx = (mx_h[...], mx_l[...])
    spectrum = dot3(halves(dot3(ty, halves(wide[...]), NN)), mx, NN)
    mine = lax.axis_index("py") * pieces_x + lax.axis_index("px")
    width = spectrum.shape[1]

    def spread_scalar(ref, place):
        return jnp.full((1, width), ref[place], jnp.float32)

    s0, s1, s2 = (spread_scalar(spacing, d) for d in range(3))
    b = spread_scalar(beta, 0)
    squares = row1[...] / (s0 * s0) + row3[pl.ds(mine, 1), :] / (s2 * s2)
    squares = squares + col2[...] * (1.0 / (s1 * s1))
    safe = jnp.where(squares > 0.0, squares, 1.0)
    volume = s0 * s1 * s2 * float(total_x * total_y * NZ)
    table = jnp.exp(safe * (-(np.pi**2) / (b * b))) / (safe * (np.pi * volume))
    table = table * (rowm[pl.ds(mine, 1), :] * colm[...])
    spectrum = spectrum * jnp.where(squares > 0.0, table, 0.0)
    wide[...] = dot3(ty, halves(dot3(halves(spectrum), mx, NT)), TN)
    turned[...] = jnp.zeros_like(turned)
    for narrow_rows, wide_rows, own, lanes in corners():
        turned[narrow_rows, own] = wide[wide_rows, lanes]
    sent[...] = turned[...].T


def gather_kernel(cells, offs, charge, spacing, got, tz_h, tz_l, out, win_h, win_l):
    window = dot3(halves(got[...].T), (tz_h[...], tz_l[...]), NN)
    win_h[...], win_l[...] = halves(window)

    @pl.loop(0, charge.shape[1] // TILE)
    def _(step):
        span = pl.ds(pl.multiple_of(step * TILE, TILE), TILE)
        near = Stencil(cells, offs, span)
        amount = charge[:, span]
        views = (win_h[...], win_l[...])
        level = dot3(views, halves(pick(near.z, near.values[2])), NN)
        tilt = dot3(views, halves(pick(near.z, near.slopes[2])), NN)
        row_x, tilt_x = pick(near.x, near.values[0]), pick(near.x, near.slopes[0])
        row_y, tilt_y = pick(near.y, near.values[1]), pick(near.y, near.slopes[1])

        def over_x(rows, field):
            total = rows[0:1] * field[0:CY]
            for x in range(1, SPAN):
                total = total + rows[x : x + 1] * field[x * CY : (x + 1) * CY]
            return total

        plain, along_x, along_z = over_x(row_x, level), over_x(tilt_x, level), over_x(row_x, tilt)
        rim_x, rim_tx = pick(near.rim_x, near.values[0]), pick(near.rim_x, near.slopes[0])
        rim_y, rim_ty = pick(near.rim_y, near.values[1]), pick(near.rim_y, near.slopes[1])
        rim_level, rim_tilt = level[MAIN:], tilt[MAIN:]

        def both(main, rim):
            return jnp.sum(main, axis=0, keepdims=True) + jnp.sum(rim, axis=0, keepdims=True)

        sampled = both(plain * row_y, rim_level * rim_x * rim_y)
        grads = (
            both(along_x * row_y, rim_level * rim_tx * rim_y),
            both(plain * tilt_y, rim_level * rim_x * rim_ty),
            both(along_z * row_y, rim_tilt * rim_x * rim_y),
        )
        for d in range(3):
            scale = jnp.full((1, TILE), spacing[d], jnp.float32)
            out[pl.ds(d, 1), span] = -amount * grads[d] / scale
        out[pl.ds(3, 1), span] = 0.5 * amount * sampled


def signed(length):
    index = np.arange(length)
    return np.where(2 * index < length, index, index - length)


def moduli(length):
    return 1.0 / ((2.0 + np.cos(2.0 * np.pi / length * np.arange(length))) / 3.0) ** 2


def middle_tables(pieces_x, pieces_y):
    pieces = pieces_x * pieces_y
    slice_z = NZ // pieces
    total_x, total_y = CX * pieces_x, CY * pieces_y
    rim = np.zeros((total_y, pieces_y, RIM))
    starts = CY * (np.arange(pieces_y) + 1)
    places = starts[:, None] + np.arange(RIM - 1)[None, :]
    rim[:, :, : RIM - 1] = cas(places.reshape(-1), total_y).reshape(total_y, pieces_y, RIM - 1)
    ty = np.concatenate([cas(np.arange(total_y), total_y), rim.reshape(total_y, -1)], axis=1)
    places = (np.arange(SPAN)[:, None] + CX * np.arange(pieces_x)[None, :]).reshape(-1)
    mx = np.kron(cas(places, total_x).T, np.eye(slice_z))
    depth = -(-mx.shape[0] // 128) * 128
    mx = np.concatenate([mx, np.zeros((depth - mx.shape[0], mx.shape[1]))], axis=0)
    row1 = np.repeat((signed(total_x) / total_x) ** 2, slice_z)[None, :]
    row3 = np.tile(((signed(NZ) / NZ) ** 2).reshape(pieces, slice_z), (1, total_x))
    rowm = np.tile(moduli(NZ).reshape(pieces, slice_z), (1, total_x))
    rowm = rowm * np.repeat(moduli(total_x), slice_z)[None, :]
    col2 = ((signed(total_y) / total_y) ** 2)[:, None]
    colm = moduli(total_y)[:, None]
    plain = tuple(jnp.asarray(t, jnp.float32) for t in (row1, row3, rowm, col2, colm))
    return constant_halves(ty) + constant_halves(mx) + plain


def in_vmem(count):
    return [pl.BlockSpec(memory_space=pltpu.VMEM)] * count


def local(base_cell, cell_offset, charges, spacing, ewald_beta):
    pieces_x = lax.axis_size("px")
    pieces_y = lax.axis_size("py")
    pieces = pieces_x * pieces_y
    cells = base_cell.reshape(-1, 3).T
    offs = cell_offset.reshape(-1, 3).T
    charge = charges.reshape(1, -1)
    tz = constant_halves(cas(np.arange(NZ), NZ))
    params = pltpu.CompilerParams(vmem_limit_bytes=VMEM_LIMIT)
    scalars = pl.BlockSpec(memory_space=pltpu.SMEM)

    def trade(tensor):
        blocks = tensor.reshape(pieces, NZ // pieces, ROWS)
        got = lax.all_to_all(blocks, ("py", "px"), split_axis=0, concat_axis=0, tiled=True)
        return got.reshape(NZ, ROWS)

    field = jax.ShapeDtypeStruct((NZ, ROWS), jnp.float32)
    spectrum = pl.pallas_call(
        spread_kernel,
        out_shape=field,
        in_specs=in_vmem(5),
        out_specs=pl.BlockSpec(memory_space=pltpu.VMEM),
        scratch_shapes=[pltpu.VMEM((ROWS, NZ), jnp.float32)],
        compiler_params=params,
        name="spread",
    )(cells, offs, charge, *tz)
    tables = middle_tables(pieces_x, pieces_y)
    spectrum = pl.pallas_call(
        functools.partial(middle_kernel, pieces_x, pieces_y),
        out_shape=field,
        in_specs=in_vmem(1) + [scalars, scalars] + in_vmem(len(tables)),
        out_specs=pl.BlockSpec(memory_space=pltpu.VMEM),
        scratch_shapes=[
            pltpu.VMEM((ROWS, NZ), jnp.float32),
            pltpu.VMEM((tables[0].shape[1], tables[2].shape[0]), jnp.float32),
        ],
        compiler_params=params,
        name="middle",
    )(trade(spectrum), spacing, ewald_beta, *tables)
    results = pl.pallas_call(
        gather_kernel,
        out_shape=jax.ShapeDtypeStruct((4, charge.shape[1]), jnp.float32),
        in_specs=in_vmem(3) + [scalars] + in_vmem(3),
        out_specs=pl.BlockSpec(memory_space=pltpu.VMEM),
        scratch_shapes=[pltpu.VMEM((ROWS, NZ), jnp.bfloat16)] * 2,
        compiler_params=params,
        name="gather",
    )(cells, offs, charge, spacing, trade(spectrum), *tz)
    return results[:3].T.reshape(base_cell.shape), results[3].reshape(charges.shape)


def solution(mesh):
    placed = (P("px", "py", None, None), P("px", "py", None, None), P("px", "py", None), P(), P())
    return jax.shard_map(
        local,
        mesh=mesh,
        in_specs=placed,
        out_specs=(P("px", "py", None, None), P("px", "py", None)),
        check_vma=False,
    )
```

```python
import functools

import jax
import jax.numpy as jnp
import numpy as np
from jax import lax
from jax.experimental import pallas as pl
from jax.experimental.pallas import tpu as pltpu
from jax.sharding import PartitionSpec as P

CX = 16
CY = 16
NZ = 256
SPAN = CX + 3
RIM = 4
MAIN = SPAN * CY
ROWS = -(-(MAIN + SPAN * RIM) // 128) * 128
TILE = 512
VMEM_LIMIT = 60 * 1024 * 1024
NN = (((1,), (0,)), ((), ()))
NT = (((1,), (1,)), ((), ()))
TN = (((0,), (0,)), ((), ()))


def cas(positions, length):
    angles = 2.0 * np.pi / length * (np.outer(np.arange(length), positions) % length)
    return np.cos(angles) + np.sin(angles)


def halves(value):
    high = value.astype(jnp.bfloat16)
    return high, (value - high.astype(jnp.float32)).astype(jnp.bfloat16)


def constant_halves(table):
    table = np.asarray(table, np.float32)
    high = table.astype(jnp.bfloat16)
    return jnp.asarray(high), jnp.asarray((table - high.astype(np.float32)).astype(jnp.bfloat16))


def dot3(left, right, dims):
    def product(a, b):
        return lax.dot_general(a, b, dims, preferred_element_type=jnp.float32)

    return product(left[0], right[0]) + (product(left[0], right[1]) + product(left[1], right[0]))


def spline_values(t):
    rest = 1.0 - t
    square = t * t
    cube = square * t
    return (
        rest * rest * rest / 6.0,
        (3.0 * cube - 6.0 * square + 4.0) / 6.0,
        (-3.0 * cube + 3.0 * square + 3.0 * t + 1.0) / 6.0,
        cube / 6.0,
    )


def spline_slopes(t):
    rest = 1.0 - t
    square = t * t
    return (-0.5 * rest * rest, 1.5 * square - 2.0 * t, -1.5 * square + t + 0.5, 0.5 * square)


def pick(masks, weights):
    chosen = jnp.where(masks[3], weights[3], 0.0)
    for step in (2, 1, 0):
        chosen = jnp.where(masks[step], weights[step], chosen)
    return chosen


def masks_of(slots, start):
    steps = slots - start
    return [steps == step for step in range(4)]


def rows_iota(rows, width):
    return lax.broadcasted_iota(jnp.int32, (rows, width), 0)


class Stencil:
    def __init__(self, cells, offs, span):
        near_x = cells[0, :, span] - lax.axis_index("px") * CX
        near_y = cells[1, :, span] - lax.axis_index("py") * CY
        near_z = cells[2, :, span]
        width = near_x.shape[1]
        rim = rows_iota(ROWS - MAIN, width)
        self.x = masks_of(rows_iota(24, width), near_x)
        self.y = masks_of(rows_iota(CY, width), near_y)
        self.rim_x = masks_of(rim // RIM, near_x)
        self.rim_y = masks_of(CY + rim % RIM, near_y)
        steps = (rows_iota(NZ, width) - near_z) & (NZ - 1)
        self.z = [steps == step for step in range(4)]
        self.values = [spline_values(offs[d, :, span]) for d in range(3)]
        self.slopes = [spline_slopes(offs[d, :, span]) for d in range(3)]


def exchange(pieces_x, src, dst, send_sem, recv_sem):
    pieces = src.shape[0]
    mine = lax.axis_index("py") * pieces_x + lax.axis_index("px")

    def copy(step):
        peer = (mine + step) % pieces
        return pltpu.make_async_remote_copy(
            src_ref=src.at[peer],
            dst_ref=dst.at[mine],
            send_sem=send_sem.at[step],
            recv_sem=recv_sem.at[step],
            device_id=(peer % pieces_x, peer // pieces_x),
            device_id_type=pl.DeviceIdType.MESH,
        )

    @pl.loop(1, pieces)
    def _(step):
        copy(step).start()

    dst[mine] = src[mine]

    @pl.loop(1, pieces)
    def _(step):
        copy(step).wait()


def field_kernel(
    pieces_x, pieces_y, cells, offs, charge, spacing, beta, tz_h, tz_l, ty_h, ty_l, mx_hbm_h,
    mx_hbm_l, row1, row3, rowm, col2, colm, out, grid, wide, mx_h, mx_l, src, dst, back, home,
    table_sem, send_sem, recv_sem,
):
    pieces = pieces_x * pieces_y
    slice_z = NZ // pieces
    mine = lax.axis_index("py") * pieces_x + lax.axis_index("px")
    loads = [
        pltpu.make_async_copy(mx_hbm_h, mx_h, table_sem.at[0]),
        pltpu.make_async_copy(mx_hbm_l, mx_l, table_sem.at[1]),
    ]
    for load in loads:
        load.start()
    barrier = pltpu.get_barrier_semaphore()

    @pl.loop(1, pieces)
    def _(step):
        peer = (mine + step) % pieces
        pl.semaphore_signal(
            barrier,
            inc=1,
            device_id=(peer % pieces_x, peer // pieces_x),
            device_id_type=pl.DeviceIdType.MESH,
        )

    grid[...] = jnp.zeros_like(grid)

    @pl.loop(0, charge.shape[1] // TILE)
    def _(step):
        span = pl.ds(pl.multiple_of(step * TILE, TILE), TILE)
        near = Stencil(cells, offs, span)
        amount = charge[:, span]
        row_x = pick(near.x, [w * amount for w in near.values[0]])
        row_y = pick(near.y, near.values[1])
        rim = pick(near.rim_x, [w * amount for w in near.values[0]]) * pick(
            near.rim_y, near.values[1]
        )
        planes = jnp.concatenate([row_x[x : x + 1] * row_y for x in range(SPAN)] + [rim], axis=0)
        grid[...] += dot3(halves(planes), halves(pick(near.z, near.values[2])), NT)

    src[...] = dot3((tz_h[...], tz_l[...]), halves(grid[...]), NT).reshape(src.shape)
    pl.semaphore_wait(barrier, pieces - 1)
    exchange(pieces_x, src, dst, send_sem.at[0], recv_sem.at[0])

    chunk = pieces_x * slice_z
    total_x = CX * pieces_x
    total_y = CY * pieces_y

    def corners():
        for x in range(SPAN):
            for j in range(pieces_y):
                lanes = pl.ds(x * chunk, chunk)
                own = pl.ds(j * chunk, chunk)
                yield pl.ds(x * CY, CY), pl.ds(j * CY, CY), own, lanes
                yield pl.ds(MAIN + x * RIM, RIM), pl.ds(total_y + j * RIM, RIM), own, lanes

    turned = grid
    turned[...] = dst[...].reshape(NZ, ROWS).T
    wide[...] = jnp.zeros_like(wide)
    for narrow_rows, wide_rows, own, lanes in corners():
        wide[wide_rows, lanes] = turned[narrow_rows, own]
    ty = (ty_h[...], ty_l[...])
    for load in loads:
        load.wait()
    mx = (mx_h[...], mx_l[...])
    spectrum = dot3(halves(dot3(ty, halves(wide[...]), NN)), mx, NN)
    width = spectrum.shape[1]

    def spread_scalar(ref, place):
        return jnp.full((1, width), ref[place], jnp.float32)

    s0, s1, s2 = (spread_scalar(spacing, d) for d in range(3))
    b = spread_scalar(beta, 0)
    squares = row1[...] / (s0 * s0) + row3[pl.ds(mine, 1), :] / (s2 * s2)
    squares = squares + col2[...] * (1.0 / (s1 * s1))
    safe = jnp.where(squares > 0.0, squares, 1.0)
    volume = s0 * s1 * s2 * float(total_x * total_y * NZ)
    table = jnp.exp(safe * (-(np.pi**2) / (b * b))) / (safe * (np.pi * volume))
    table = table * (rowm[pl.ds(mine, 1), :] * colm[...])
    spectrum = spectrum * jnp.where(squares > 0.0, table, 0.0)
    wide[...] = dot3(ty, halves(dot3(halves(spectrum), mx, NT)), TN)
    turned[...] = jnp.zeros_like(turned)
    for narrow_rows, wide_rows, own, lanes in corners():
        turned[narrow_rows, own] = wide[wide_rows, lanes]
    back[...] = turned[...].T.reshape(back.shape)
    exchange(pieces_x, back, home, send_sem.at[1], recv_sem.at[1])
    out[...] = home[...].reshape(NZ, ROWS)


def gather_kernel(cells, offs, charge, spacing, got, tz_h, tz_l, forces, energy, win_h, win_l):
    window = dot3(halves(got[...].T), (tz_h[...], tz_l[...]), NN)
    win_h[...], win_l[...] = halves(window)

    @pl.loop(0, charge.shape[1] // TILE)
    def _(step):
        span = pl.ds(pl.multiple_of(step * TILE, TILE), TILE)
        near = Stencil(cells, offs, span)
        amount = charge[:, span]
        views = (win_h[...], win_l[...])
        level = dot3(views, halves(pick(near.z, near.values[2])), NN)
        tilt = dot3(views, halves(pick(near.z, near.slopes[2])), NN)
        row_x, tilt_x = pick(near.x, near.values[0]), pick(near.x, near.slopes[0])
        row_y, tilt_y = pick(near.y, near.values[1]), pick(near.y, near.slopes[1])

        def over_x(rows, field):
            total = rows[0:1] * field[0:CY]
            for x in range(1, SPAN):
                total = total + rows[x : x + 1] * field[x * CY : (x + 1) * CY]
            return total

        plain, along_x, along_z = over_x(row_x, level), over_x(tilt_x, level), over_x(row_x, tilt)
        rim_x, rim_tx = pick(near.rim_x, near.values[0]), pick(near.rim_x, near.slopes[0])
        rim_y, rim_ty = pick(near.rim_y, near.values[1]), pick(near.rim_y, near.slopes[1])
        rim_level, rim_tilt = level[MAIN:], tilt[MAIN:]

        def both(main, rim):
            return jnp.sum(main, axis=0, keepdims=True) + jnp.sum(rim, axis=0, keepdims=True)

        sampled = both(plain * row_y, rim_level * rim_x * rim_y)
        grads = (
            both(along_x * row_y, rim_level * rim_tx * rim_y),
            both(plain * tilt_y, rim_level * rim_x * rim_ty),
            both(along_z * row_y, rim_tilt * rim_x * rim_y),
        )
        for d in range(3):
            scale = jnp.full((1, TILE), spacing[d], jnp.float32)
            forces[d, :, span] = -amount * grads[d] / scale
        energy[:, span] = 0.5 * amount * sampled


def signed(length):
    index = np.arange(length)
    return np.where(2 * index < length, index, index - length)


def moduli(length):
    return 1.0 / ((2.0 + np.cos(2.0 * np.pi / length * np.arange(length))) / 3.0) ** 2


def middle_tables(pieces_x, pieces_y):
    pieces = pieces_x * pieces_y
    slice_z = NZ // pieces
    total_x, total_y = CX * pieces_x, CY * pieces_y
    rim = np.zeros((total_y, pieces_y, RIM))
    starts = CY * (np.arange(pieces_y) + 1)
    places = starts[:, None] + np.arange(RIM - 1)[None, :]
    rim[:, :, : RIM - 1] = cas(places.reshape(-1), total_y).reshape(total_y, pieces_y, RIM - 1)
    ty = np.concatenate([cas(np.arange(total_y), total_y), rim.reshape(total_y, -1)], axis=1)
    places = (np.arange(SPAN)[:, None] + CX * np.arange(pieces_x)[None, :]).reshape(-1)
    mx = np.kron(cas(places, total_x).T, np.eye(slice_z))
    depth = -(-mx.shape[0] // 128) * 128
    mx = np.concatenate([mx, np.zeros((depth - mx.shape[0], mx.shape[1]))], axis=0)
    row1 = np.repeat((signed(total_x) / total_x) ** 2, slice_z)[None, :]
    row3 = np.tile(((signed(NZ) / NZ) ** 2).reshape(pieces, slice_z), (1, total_x))
    rowm = np.tile(moduli(NZ).reshape(pieces, slice_z), (1, total_x))
    rowm = rowm * np.repeat(moduli(total_x), slice_z)[None, :]
    col2 = ((signed(total_y) / total_y) ** 2)[:, None]
    colm = moduli(total_y)[:, None]
    plain = tuple(jnp.asarray(t, jnp.float32) for t in (row1, row3, rowm, col2, colm))
    return constant_halves(ty) + constant_halves(mx) + plain


def local(base_cell, cell_offset, charges, spacing, ewald_beta):
    pieces_x = lax.axis_size("px")
    pieces_y = lax.axis_size("py")
    pieces = pieces_x * pieces_y
    charge = charges.reshape(1, -1)
    atoms = charge.shape[1]
    cells = jnp.transpose(base_cell, (0, 3, 1, 2)).reshape(3, 1, atoms)
    offs = jnp.transpose(cell_offset, (0, 3, 1, 2)).reshape(3, 1, atoms)
    tz = constant_halves(cas(np.arange(NZ), NZ))
    tables = middle_tables(pieces_x, pieces_y)
    vmem = pl.BlockSpec(memory_space=pltpu.VMEM)
    scalars = pl.BlockSpec(memory_space=pltpu.SMEM)
    anywhere = pl.BlockSpec(memory_space=pl.ANY)
    blocks = pltpu.VMEM((pieces, NZ // pieces, ROWS), jnp.float32)
    field = pl.pallas_call(
        functools.partial(field_kernel, pieces_x, pieces_y),
        out_shape=jax.ShapeDtypeStruct((NZ, ROWS), jnp.float32),
        in_specs=[vmem] * 3 + [scalars] * 2 + [vmem] * 4 + [anywhere] * 2 + [vmem] * 5,
        out_specs=vmem,
        scratch_shapes=[
            pltpu.VMEM((ROWS, NZ), jnp.float32),
            pltpu.VMEM((tables[0].shape[1], tables[2].shape[0]), jnp.float32),
            pltpu.VMEM(tables[2].shape, jnp.bfloat16),
            pltpu.VMEM(tables[2].shape, jnp.bfloat16),
            blocks,
            blocks,
            blocks,
            blocks,
            pltpu.SemaphoreType.DMA((2,)),
            pltpu.SemaphoreType.DMA((2, pieces)),
            pltpu.SemaphoreType.DMA((2, pieces)),
        ],
        compiler_params=pltpu.CompilerParams(
            vmem_limit_bytes=VMEM_LIMIT, collective_id=0, has_side_effects=True
        ),
        name="field",
    )(cells, offs, charge, spacing, ewald_beta, *tz, *tables)
    forces, energy = pl.pallas_call(
        gather_kernel,
        out_shape=(
            jax.ShapeDtypeStruct((3, 1, atoms), jnp.float32),
            jax.ShapeDtypeStruct((1, atoms), jnp.float32),
        ),
        in_specs=[vmem] * 3 + [scalars] + [vmem] * 3,
        out_specs=(vmem, vmem),
        scratch_shapes=[pltpu.VMEM((ROWS, NZ), jnp.bfloat16)] * 2,
        compiler_params=pltpu.CompilerParams(vmem_limit_bytes=VMEM_LIMIT),
        name="gather",
    )(cells, offs, charge, spacing, field, *tz)
    forces = jnp.transpose(forces.reshape(1, 3, 1, atoms), (0, 2, 3, 1))
    return forces, energy.reshape(charges.shape)


def solution(mesh):
    placed = (P("px", "py", None, None), P("px", "py", None, None), P("px", "py", None), P(), P())
    return jax.shard_map(
        local,
        mesh=mesh,
        in_specs=placed,
        out_specs=(P("px", "py", None, None), P("px", "py", None)),
        check_vma=False,
    )
```

```python
import functools

import jax
import jax.numpy as jnp
import numpy as np
from jax import lax
from jax.experimental import pallas as pl
from jax.experimental.pallas import tpu as pltpu
from jax.sharding import PartitionSpec as P

CX = 16
CY = 16
NZ = 256
SPAN = CX + 3
RIM = 4
MAIN = SPAN * CY
CORE = CX * CY
ROWS = -(-(MAIN + SPAN * RIM) // 128) * 128
TILE = 512
VMEM_LIMIT = 60 * 1024 * 1024
NN = (((1,), (0,)), ((), ()))
NT = (((1,), (1,)), ((), ()))
TN = (((0,), (0,)), ((), ()))


def cas(positions, length):
    angles = 2.0 * np.pi / length * (np.outer(np.arange(length), positions) % length)
    return np.cos(angles) + np.sin(angles)


def halves(value):
    high = value.astype(jnp.bfloat16)
    return high, (value - high.astype(jnp.float32)).astype(jnp.bfloat16)


def constant_halves(table):
    table = np.asarray(table, np.float32)
    high = table.astype(jnp.bfloat16)
    return jnp.asarray(high), jnp.asarray((table - high.astype(np.float32)).astype(jnp.bfloat16))


def dot3(left, right, dims):
    def product(a, b):
        return lax.dot_general(a, b, dims, preferred_element_type=jnp.float32)

    if dims == TN:
        cross = product(left[0], right[1]) + product(left[1], right[0])
        return product(left[0], right[0]) + cross
    rows = left[0].shape[0]
    stacked = product(jnp.concatenate(left, axis=0), right[0])
    return stacked[:rows] + (stacked[rows:] + product(left[0], right[1]))


def spline_values(t):
    rest = 1.0 - t
    square = t * t
    cube = square * t
    return (
        rest * rest * rest / 6.0,
        (3.0 * cube - 6.0 * square + 4.0) / 6.0,
        (-3.0 * cube + 3.0 * square + 3.0 * t + 1.0) / 6.0,
        cube / 6.0,
    )


def spline_slopes(t):
    rest = 1.0 - t
    square = t * t
    return (-0.5 * rest * rest, 1.5 * square - 2.0 * t, -1.5 * square + t + 0.5, 0.5 * square)


def pick(masks, weights):
    chosen = jnp.where(masks[3], weights[3], 0.0)
    for step in (2, 1, 0):
        chosen = jnp.where(masks[step], weights[step], chosen)
    return chosen


def masks_of(slots, start):
    steps = slots - start
    return [steps == step for step in range(4)]


def rows_iota(rows, width):
    return lax.broadcasted_iota(jnp.int32, (rows, width), 0)


class Stencil:
    def __init__(self, cells, offs, span):
        self.near_x = cells[0, :, span] - lax.axis_index("px") * CX
        self.near_y = cells[1, :, span] - lax.axis_index("py") * CY
        self.near_z = cells[2, :, span]
        self.width = self.near_x.shape[1]
        self.t = [offs[d, :, span] for d in range(3)]

    def x(self):
        return masks_of(rows_iota(24, self.width), self.near_x)

    def y(self):
        return masks_of(rows_iota(CY, self.width), self.near_y)

    def rim(self):
        rim = rows_iota(ROWS - MAIN, self.width)
        return masks_of(rim // RIM, self.near_x), masks_of(CY + rim % RIM, self.near_y)

    def z(self):
        steps = (rows_iota(NZ, self.width) - self.near_z) & (NZ - 1)
        return [steps == step for step in range(4)]

    def values(self, d):
        return spline_values(self.t[d])

    def slopes(self, d):
        return spline_slopes(self.t[d])


class Exchange:
    def __init__(self, pieces_x, src, dst, lanes, send_sem, recv_sem):
        self.pieces_x, self.src, self.dst, self.lanes = pieces_x, src, dst, lanes
        self.send_sem, self.recv_sem = send_sem, recv_sem
        self.pieces = src.shape[0]
        self.mine = lax.axis_index("py") * pieces_x + lax.axis_index("px")

    def copy(self, step):
        peer = (self.mine + step) % self.pieces
        return pltpu.make_async_remote_copy(
            src_ref=self.src.at[peer, :, self.lanes],
            dst_ref=self.dst.at[self.mine, :, self.lanes],
            send_sem=self.send_sem.at[step],
            recv_sem=self.recv_sem.at[step],
            device_id=(peer % self.pieces_x, peer // self.pieces_x),
            device_id_type=pl.DeviceIdType.MESH,
        )

    def put(self, value):
        self.src[:, :, self.lanes] = value.reshape(self.src.shape[:2] + (value.shape[1],))

        @pl.loop(1, self.pieces)
        def _(step):
            self.copy(step).start()

        self.dst[self.mine, :, self.lanes] = self.src[self.mine, :, self.lanes]

    def get(self):
        @pl.loop(1, self.pieces)
        def _(step):
            self.copy(step).wait()

        return self.dst[:, :, self.lanes].reshape(NZ, -1)


def kernel(
    pieces_x, pieces_y, cells, offs, charge, spacing, beta, tz_h, tz_l, ty_h, ty_l, mx_hbm_h,
    mx_hbm_l, row1, row3, rowm, col2, colm, forces, energy, grid, wide, mx_h, mx_l, rz_h, rz_l,
    dz_h, dz_l, window, part, src, dst, back, home, table_sem, send_sem, recv_sem,
):
    pieces = pieces_x * pieces_y
    slice_z = NZ // pieces
    mine = lax.axis_index("py") * pieces_x + lax.axis_index("px")
    core, edge = pl.ds(0, CORE), pl.ds(CORE, ROWS - CORE)
    loads = [
        pltpu.make_async_copy(mx_hbm_h, mx_h, table_sem.at[0]),
        pltpu.make_async_copy(mx_hbm_l, mx_l, table_sem.at[1]),
    ]
    for load in loads:
        load.start()
    barrier = pltpu.get_barrier_semaphore()

    @pl.loop(1, pieces)
    def _(step):
        peer = (mine + step) % pieces
        pl.semaphore_signal(
            barrier,
            inc=1,
            device_id=(peer % pieces_x, peer // pieces_x),
            device_id_type=pl.DeviceIdType.MESH,
        )

    def tiles(body):
        @pl.loop(0, charge.shape[1] // TILE)
        def _(step):
            span = pl.ds(pl.multiple_of(step * TILE, TILE), TILE)
            body(span, Stencil(cells, offs, span), charge[:, span])

    tz = (tz_h[...], tz_l[...])
    grid[...] = jnp.zeros_like(grid)

    def spread_core(span, near, amount):
        row_x = pick(near.x(), [w * amount for w in near.values(0)])
        row_y = pick(near.y(), near.values(1))
        planes = jnp.concatenate([row_x[x : x + 1] * row_y for x in range(CX)], axis=0)
        profile = halves(pick(near.z(), near.values(2)))
        rz_h[:, span], rz_l[:, span] = profile
        grid[core, :] += dot3(halves(planes), profile, NT)

    tiles(spread_core)
    ahead = [
        Exchange(pieces_x, src, dst, lanes, send_sem.at[k], recv_sem.at[k])
        for k, lanes in enumerate((core, edge))
    ]
    value = dot3(tz, halves(grid[core, :]), NT)
    pl.semaphore_wait(barrier, pieces - 1)
    ahead[0].put(value)

    def spread_edge(span, near, amount):
        heavy = [w * amount for w in near.values(0)]
        row_x = pick(near.x(), heavy)
        row_y = pick(near.y(), near.values(1))
        rim_x, rim_y = near.rim()
        rim = pick(rim_x, heavy) * pick(rim_y, near.values(1))
        planes = [row_x[x : x + 1] * row_y for x in range(CX, SPAN)] + [rim]
        planes = jnp.concatenate(planes, axis=0)
        grid[edge, :] += dot3(halves(planes), (rz_h[:, span], rz_l[:, span]), NT)

    tiles(spread_edge)
    ahead[1].put(dot3(tz, halves(grid[edge, :]), NT))

    def slopes_z(span, near, amount):
        dz_h[:, span], dz_l[:, span] = halves(pick(near.z(), near.slopes(2)))

    tiles(slopes_z)

    chunk = pieces_x * slice_z
    total_x = CX * pieces_x
    total_y = CY * pieces_y
    split = CX * chunk
    turned = grid

    def main_corners(planes):
        for x in planes:
            for j in range(pieces_y):
                lanes, own = pl.ds(x * chunk, chunk), pl.ds(j * chunk, chunk)
                yield (pl.ds(x * CY, CY), own), (pl.ds(j * CY, CY), lanes)

    def rim_corners():
        for x in range(SPAN):
            for j in range(pieces_y):
                lanes, own = pl.ds(x * chunk, chunk), pl.ds(j * chunk, chunk)
                yield (pl.ds(MAIN + x * RIM, RIM), own), (pl.ds(total_y + j * RIM, RIM), lanes)

    def edge_corners():
        yield from main_corners(range(CX, SPAN))
        yield from rim_corners()

    tails = pl.ds(split, wide.shape[1] - split)
    wide[:, tails] = jnp.zeros((wide.shape[0], wide.shape[1] - split), jnp.float32)
    ty = (ty_h[:, :total_y], ty_l[:, :total_y])
    ty_rim = (ty_h[:, total_y:], ty_l[:, total_y:])
    turned[core, :] = ahead[0].get().T
    for narrow, broad in main_corners(range(CX)):
        wide[broad] = turned[narrow]
    first = dot3(ty, halves(wide[:total_y, :split]), NN)
    turned[edge, :] = ahead[1].get().T
    for narrow, broad in edge_corners():
        wide[broad] = turned[narrow]
    last = dot3(ty, halves(wide[:total_y, split:]), NN)
    mixed = jnp.concatenate([first, last], axis=1) + dot3(ty_rim, halves(wide[total_y:, :]), NN)
    for load in loads:
        load.wait()
    mx = (mx_h[...], mx_l[...])
    spectrum = dot3(halves(mixed), mx, NN)
    width = spectrum.shape[1]

    def spread_scalar(ref, place):
        return jnp.full((1, width), ref[place], jnp.float32)

    s0, s1, s2 = (spread_scalar(spacing, d) for d in range(3))
    b = spread_scalar(beta, 0)
    squares = row1[...] / (s0 * s0) + row3[pl.ds(mine, 1), :] / (s2 * s2)
    squares = squares + col2[...] * (1.0 / (s1 * s1))
    safe = jnp.where(squares > 0.0, squares, 1.0)
    volume = s0 * s1 * s2 * float(total_x * total_y * NZ)
    table = jnp.exp(safe * (-(np.pi**2) / (b * b))) / (safe * (np.pi * volume))
    table = table * (rowm[pl.ds(mine, 1), :] * colm[...])
    spectrum = spectrum * jnp.where(squares > 0.0, table, 0.0)
    mixed = halves(dot3(halves(spectrum), mx, NT))
    after = [
        Exchange(pieces_x, back, home, lanes, send_sem.at[2 + k], recv_sem.at[2 + k])
        for k, lanes in enumerate((core, edge))
    ]
    wide[total_y:, :] = dot3(ty_rim, mixed, TN)
    wide[:total_y, split:] = dot3(ty, tuple(half[:, split:] for half in mixed), TN)
    turned[edge, :] = jnp.zeros((ROWS - CORE, NZ), jnp.float32)
    for narrow, broad in edge_corners():
        turned[narrow] = wide[broad]
    after[1].put(turned[edge, :].T)
    wide[:total_y, :split] = dot3(ty, tuple(half[:, :split] for half in mixed), TN)
    for narrow, broad in main_corners(range(CX)):
        turned[narrow] = wide[broad]
    after[0].put(turned[core, :].T)

    def fields(rows, span):
        def sampled_with(high, low):
            stacked = jnp.dot(
                window[: 2 * rows], high[:, span], preferred_element_type=jnp.float32
            )
            rest = jnp.dot(window[:rows], low[:, span], preferred_element_type=jnp.float32)
            return stacked[:rows] + (stacked[rows:] + rest)

        return sampled_with(rz_h, rz_l), sampled_with(dz_h, dz_l)

    def over_x(planes, rows, field):
        total = rows[planes[0] : planes[0] + 1] * field[0:CY]
        for k, x in enumerate(planes[1:], 1):
            total = total + rows[x : x + 1] * field[k * CY : (k + 1) * CY]
        return total

    def four_sums(planes, near, level, tilt):
        masks_x, masks_y = near.x(), near.y()
        row_x, tilt_x = pick(masks_x, near.values(0)), pick(masks_x, near.slopes(0))
        row_y, tilt_y = pick(masks_y, near.values(1)), pick(masks_y, near.slopes(1))
        plain = over_x(planes, row_x, level)
        return [
            jnp.sum(product, axis=0, keepdims=True)
            for product in (
                over_x(planes, tilt_x, level) * row_y,
                plain * tilt_y,
                over_x(planes, row_x, tilt) * row_y,
                plain * row_y,
            )
        ]

    def set_window(got):
        field = halves(dot3(halves(got.T), tz, NN))
        window[: 2 * got.shape[1]] = jnp.concatenate(field, axis=0)

    def gather_edge(span, near, amount):
        level, tilt = fields(ROWS - CORE, span)
        sums = four_sums(range(CX, SPAN), near, level, tilt)
        masks_x, masks_y = near.rim()
        row_x, tilt_x = pick(masks_x, near.values(0)), pick(masks_x, near.slopes(0))
        row_y, tilt_y = pick(masks_y, near.values(1)), pick(masks_y, near.slopes(1))
        level, tilt = level[MAIN - CORE :], tilt[MAIN - CORE :]
        flat = row_x * row_y
        extra = (level * tilt_x * row_y, level * row_x * tilt_y, tilt * flat, level * flat)
        for d in range(4):
            part[d, :, span] = sums[d] + jnp.sum(extra[d], axis=0, keepdims=True)

    set_window(after[1].get())
    tiles(gather_edge)

    def gather_core(span, near, amount):
        sums = four_sums(range(CX), near, *fields(CORE, span))
        for d in range(3):
            scale = jnp.full((1, TILE), spacing[d], jnp.float32)
            forces[d, :, span] = -amount * (sums[d] + part[d, :, span]) / scale
        energy[:, span] = 0.5 * amount * (sums[3] + part[3, :, span])

    set_window(after[0].get())
    tiles(gather_core)


def signed(length):
    index = np.arange(length)
    return np.where(2 * index < length, index, index - length)


def moduli(length):
    return 1.0 / ((2.0 + np.cos(2.0 * np.pi / length * np.arange(length))) / 3.0) ** 2


def middle_tables(pieces_x, pieces_y):
    pieces = pieces_x * pieces_y
    slice_z = NZ // pieces
    total_x, total_y = CX * pieces_x, CY * pieces_y
    rim = np.zeros((total_y, pieces_y, RIM))
    starts = CY * (np.arange(pieces_y) + 1)
    places = starts[:, None] + np.arange(RIM - 1)[None, :]
    rim[:, :, : RIM - 1] = cas(places.reshape(-1), total_y).reshape(total_y, pieces_y, RIM - 1)
    ty = np.concatenate([cas(np.arange(total_y), total_y), rim.reshape(total_y, -1)], axis=1)
    places = (np.arange(SPAN)[:, None] + CX * np.arange(pieces_x)[None, :]).reshape(-1)
    mx = np.kron(cas(places, total_x).T, np.eye(slice_z))
    depth = -(-mx.shape[0] // 128) * 128
    mx = np.concatenate([mx, np.zeros((depth - mx.shape[0], mx.shape[1]))], axis=0)
    row1 = np.repeat((signed(total_x) / total_x) ** 2, slice_z)[None, :]
    row3 = np.tile(((signed(NZ) / NZ) ** 2).reshape(pieces, slice_z), (1, total_x))
    rowm = np.tile(moduli(NZ).reshape(pieces, slice_z), (1, total_x))
    rowm = rowm * np.repeat(moduli(total_x), slice_z)[None, :]
    col2 = ((signed(total_y) / total_y) ** 2)[:, None]
    colm = moduli(total_y)[:, None]
    plain = tuple(jnp.asarray(t, jnp.float32) for t in (row1, row3, rowm, col2, colm))
    return constant_halves(ty) + constant_halves(mx) + plain


def local(base_cell, cell_offset, charges, spacing, ewald_beta):
    pieces_x = lax.axis_size("px")
    pieces_y = lax.axis_size("py")
    pieces = pieces_x * pieces_y
    charge = charges.reshape(1, -1)
    atoms = charge.shape[1]
    cells = jnp.transpose(base_cell, (0, 3, 1, 2)).reshape(3, 1, atoms)
    offs = jnp.transpose(cell_offset, (0, 3, 1, 2)).reshape(3, 1, atoms)
    tz = constant_halves(cas(np.arange(NZ), NZ))
    tables = middle_tables(pieces_x, pieces_y)
    vmem = pl.BlockSpec(memory_space=pltpu.VMEM)
    scalars = pl.BlockSpec(memory_space=pltpu.SMEM)
    anywhere = pl.BlockSpec(memory_space=pl.ANY)
    blocks = pltpu.VMEM((pieces, NZ // pieces, ROWS), jnp.float32)
    profile = pltpu.VMEM((NZ, atoms), jnp.bfloat16)
    forces, energy = pl.pallas_call(
        functools.partial(kernel, pieces_x, pieces_y),
        out_shape=(
            jax.ShapeDtypeStruct((3, 1, atoms), jnp.float32),
            jax.ShapeDtypeStruct((1, atoms), jnp.float32),
        ),
        in_specs=[vmem] * 3 + [scalars] * 2 + [vmem] * 4 + [anywhere] * 2 + [vmem] * 5,
        out_specs=(vmem, vmem),
        scratch_shapes=[
            pltpu.VMEM((ROWS, NZ), jnp.float32),
            pltpu.VMEM((tables[0].shape[1], tables[2].shape[0]), jnp.float32),
            pltpu.VMEM(tables[2].shape, jnp.bfloat16),
            pltpu.VMEM(tables[2].shape, jnp.bfloat16),
            profile,
            profile,
            profile,
            profile,
            pltpu.VMEM((2 * CORE, NZ), jnp.bfloat16),
            pltpu.VMEM((4, 1, atoms), jnp.float32),
            blocks,
            blocks,
            blocks,
            blocks,
            pltpu.SemaphoreType.DMA((2,)),
            pltpu.SemaphoreType.DMA((4, pieces)),
            pltpu.SemaphoreType.DMA((4, pieces)),
        ],
        compiler_params=pltpu.CompilerParams(
            vmem_limit_bytes=VMEM_LIMIT, collective_id=0, has_side_effects=True
        ),
        name="ewald",
    )(cells, offs, charge, spacing, ewald_beta, *tz, *tables)
    forces = jnp.transpose(forces.reshape(1, 3, 1, atoms), (0, 2, 3, 1))
    return forces, energy.reshape(charges.shape)


def solution(mesh):
    placed = (P("px", "py", None, None), P("px", "py", None, None), P("px", "py", None), P(), P())
    return jax.shard_map(
        local,
        mesh=mesh,
        in_specs=placed,
        out_specs=(P("px", "py", None, None), P("px", "py", None)),
        check_vma=False,
    )
```

```python
import functools

import jax
import jax.numpy as jnp
import numpy as np
from jax import lax
from jax.experimental import pallas as pl
from jax.experimental.pallas import tpu as pltpu
from jax.sharding import PartitionSpec as P

CX = 16
CY = 16
NZ = 256
SPAN = CX + 3
RIM = 4
MAIN = SPAN * CY
CORE = CX * CY
ROWS = -(-(MAIN + SPAN * RIM) // 128) * 128
TILE = 512
VMEM_LIMIT = 60 * 1024 * 1024
NN = (((1,), (0,)), ((), ()))
NT = (((1,), (1,)), ((), ()))
TN = (((0,), (0,)), ((), ()))


def cas(positions, length):
    angles = 2.0 * np.pi / length * (np.outer(np.arange(length), positions) % length)
    return np.cos(angles) + np.sin(angles)


def halves(value):
    high = value.astype(jnp.bfloat16)
    return high, (value - high.astype(jnp.float32)).astype(jnp.bfloat16)


def constant_halves(table):
    table = np.asarray(table, np.float32)
    high = table.astype(jnp.bfloat16)
    return jnp.asarray(high), jnp.asarray((table - high.astype(np.float32)).astype(jnp.bfloat16))


def dot3(left, right, dims):
    def product(a, b):
        return lax.dot_general(a, b, dims, preferred_element_type=jnp.float32)

    if dims == TN:
        cross = product(left[0], right[1]) + product(left[1], right[0])
        return product(left[0], right[0]) + cross
    rows = left[0].shape[0]
    stacked = product(jnp.concatenate(left, axis=0), right[0])
    return stacked[:rows] + (stacked[rows:] + product(left[0], right[1]))


def spline_values(t):
    rest = 1.0 - t
    square = t * t
    cube = square * t
    return (
        rest * rest * rest / 6.0,
        (3.0 * cube - 6.0 * square + 4.0) / 6.0,
        (-3.0 * cube + 3.0 * square + 3.0 * t + 1.0) / 6.0,
        cube / 6.0,
    )


def spline_slopes(t):
    rest = 1.0 - t
    square = t * t
    return (-0.5 * rest * rest, 1.5 * square - 2.0 * t, -1.5 * square + t + 0.5, 0.5 * square)


def pick(masks, weights):
    chosen = jnp.where(masks[3], weights[3], 0.0)
    for step in (2, 1, 0):
        chosen = jnp.where(masks[step], weights[step], chosen)
    return chosen


def masks_of(slots, start):
    steps = slots - start
    return [steps == step for step in range(4)]


def rows_iota(rows, width):
    return lax.broadcasted_iota(jnp.int32, (rows, width), 0)


class Stencil:
    def __init__(self, cells, offs, span):
        self.near_x = cells[0, :, span] - lax.axis_index("px") * CX
        self.near_y = cells[1, :, span] - lax.axis_index("py") * CY
        self.near_z = cells[2, :, span]
        self.width = self.near_x.shape[1]
        self.t = [offs[d, :, span] for d in range(3)]

    def x(self):
        return masks_of(rows_iota(24, self.width), self.near_x)

    def y(self):
        return masks_of(rows_iota(CY, self.width), self.near_y)

    def rim(self):
        rim = rows_iota(ROWS - MAIN, self.width)
        return masks_of(rim // RIM, self.near_x), masks_of(CY + rim % RIM, self.near_y)

    def z(self):
        steps = (rows_iota(NZ, self.width) - self.near_z) & (NZ - 1)
        return [steps == step for step in range(4)]

    def values(self, d):
        return spline_values(self.t[d])

    def slopes(self, d):
        return spline_slopes(self.t[d])


class Exchange:
    def __init__(self, pieces_x, src, dst, lanes, send_sem, recv_sem):
        self.pieces_x, self.src, self.dst, self.lanes = pieces_x, src, dst, lanes
        self.send_sem, self.recv_sem = send_sem, recv_sem
        self.pieces = src.shape[0]
        self.mine = lax.axis_index("py") * pieces_x + lax.axis_index("px")

    def copy(self, step):
        peer = (self.mine + step) % self.pieces
        return pltpu.make_async_remote_copy(
            src_ref=self.src.at[peer, :, self.lanes],
            dst_ref=self.dst.at[self.mine, :, self.lanes],
            send_sem=self.send_sem.at[step],
            recv_sem=self.recv_sem.at[step],
            device_id=(peer % self.pieces_x, peer // self.pieces_x),
            device_id_type=pl.DeviceIdType.MESH,
        )

    def put(self, value):
        self.src[:, :, self.lanes] = value.reshape(self.src.shape[:2] + (value.shape[1],))

        @pl.loop(1, self.pieces)
        def _(step):
            self.copy(step).start()

        self.dst[self.mine, :, self.lanes] = self.src[self.mine, :, self.lanes]

    def get(self):
        @pl.loop(1, self.pieces)
        def _(step):
            self.copy(step).wait()

        return self.dst[:, :, self.lanes].reshape(NZ, -1)


def kernel(
    pieces_x, pieces_y, cells, offs, charge, spacing, beta, tz_h, tz_l, ty_h, ty_l, mx_hbm_h,
    mx_hbm_l, row1, row3, rowm, col2, colm, forces, energy, grid, wide, mx_h, mx_l, rz_h, rz_l,
    dz_h, dz_l, window, part, weight, src, dst, back, home, table_sem, send_sem, recv_sem,
):
    pieces = pieces_x * pieces_y
    slice_z = NZ // pieces
    mine = lax.axis_index("py") * pieces_x + lax.axis_index("px")
    half = CX // 2
    cores = [range(0, half), range(half, CX)]
    rows_of = [pl.ds(k * half * CY, half * CY) for k in range(2)] + [pl.ds(CORE, ROWS - CORE)]
    loads = [
        pltpu.make_async_copy(mx_hbm_h, mx_h, table_sem.at[0]),
        pltpu.make_async_copy(mx_hbm_l, mx_l, table_sem.at[1]),
    ]
    for load in loads:
        load.start()
    barrier = pltpu.get_barrier_semaphore()

    @pl.loop(1, pieces)
    def _(step):
        peer = (mine + step) % pieces
        pl.semaphore_signal(
            barrier,
            inc=1,
            device_id=(peer % pieces_x, peer // pieces_x),
            device_id_type=pl.DeviceIdType.MESH,
        )

    def tiles(body):
        @pl.loop(0, charge.shape[1] // TILE)
        def _(step):
            span = pl.ds(pl.multiple_of(step * TILE, TILE), TILE)
            body(span, Stencil(cells, offs, span), charge[:, span])

    tz = (tz_h[...], tz_l[...])
    grid[...] = jnp.zeros_like(grid)

    def exchanges(source, target, base):
        return [
            Exchange(pieces_x, source, target, rows, send_sem.at[base + k], recv_sem.at[base + k])
            for k, rows in enumerate(rows_of)
        ]

    def spread_edge(span, near, amount):
        heavy = [w * amount for w in near.values(0)]
        row_x = pick(near.x(), heavy)
        row_y = pick(near.y(), near.values(1))
        rim_x, rim_y = near.rim()
        rim = pick(rim_x, heavy) * pick(rim_y, near.values(1))
        planes = [row_x[x : x + 1] * row_y for x in range(CX, SPAN)] + [rim]
        profile = halves(pick(near.z(), near.values(2)))
        rz_h[:, span], rz_l[:, span] = profile
        grid[rows_of[2], :] += dot3(halves(jnp.concatenate(planes, axis=0)), profile, NT)

    def spread_core(k, span, near, amount):
        row_x = pick(near.x(), [w * amount for w in near.values(0)])
        row_y = pick(near.y(), near.values(1))
        planes = jnp.concatenate([row_x[x : x + 1] * row_y for x in cores[k]], axis=0)
        grid[rows_of[k], :] += dot3(halves(planes), (rz_h[:, span], rz_l[:, span]), NT)

    ahead = exchanges(src, dst, 0)
    tiles(spread_edge)
    value = dot3(tz, halves(grid[rows_of[2], :]), NT)
    pl.semaphore_wait(barrier, pieces - 1)
    ahead[2].put(value)
    for k in range(2):
        tiles(functools.partial(spread_core, k))
        ahead[k].put(dot3(tz, halves(grid[rows_of[k], :]), NT))

    def slopes_z(span, near, amount):
        dz_h[:, span], dz_l[:, span] = halves(pick(near.z(), near.slopes(2)))

    tiles(slopes_z)

    chunk = pieces_x * slice_z
    total_x = CX * pieces_x
    total_y = CY * pieces_y
    split = CX * chunk
    turned = grid

    def main_corners(planes):
        for x in planes:
            for j in range(pieces_y):
                lanes, own = pl.ds(x * chunk, chunk), pl.ds(j * chunk, chunk)
                yield (pl.ds(x * CY, CY), own), (pl.ds(j * CY, CY), lanes)

    def rim_corners():
        for x in range(SPAN):
            for j in range(pieces_y):
                lanes, own = pl.ds(x * chunk, chunk), pl.ds(j * chunk, chunk)
                yield (pl.ds(MAIN + x * RIM, RIM), own), (pl.ds(total_y + j * RIM, RIM), lanes)

    def edge_corners():
        yield from main_corners(range(CX, SPAN))
        yield from rim_corners()

    tails = pl.ds(split, wide.shape[1] - split)
    wide[:, tails] = jnp.zeros((wide.shape[0], wide.shape[1] - split), jnp.float32)
    ty = (ty_h[:, :total_y], ty_l[:, :total_y])
    ty_rim = (ty_h[:, total_y:], ty_l[:, total_y:])
    width = mx_h.shape[1]

    def spread_scalar(ref, place):
        return jnp.full((1, width), ref[place], jnp.float32)

    s0, s1, s2 = (spread_scalar(spacing, d) for d in range(3))
    b = spread_scalar(beta, 0)
    squares = row1[...] / (s0 * s0) + row3[pl.ds(mine, 1), :] / (s2 * s2)
    squares = squares + col2[...] * (1.0 / (s1 * s1))
    safe = jnp.where(squares > 0.0, squares, 1.0)
    volume = s0 * s1 * s2 * float(total_x * total_y * NZ)
    table = jnp.exp(safe * (-(np.pi**2) / (b * b))) / (safe * (np.pi * volume))
    table = table * (rowm[pl.ds(mine, 1), :] * colm[...])
    weight[...] = jnp.where(squares > 0.0, table, 0.0)
    for load in loads:
        load.wait()

    turned[rows_of[2], :] = ahead[2].get().T
    for narrow, broad in edge_corners():
        wide[broad] = turned[narrow]
    mixed = dot3(ty_rim, halves(wide[total_y:, :]), NN)
    last = dot3(ty, halves(wide[:total_y, split:]), NN)
    mixed = jnp.concatenate([mixed[:, :split], mixed[:, split:] + last], axis=1)
    spectrum = dot3(halves(mixed), (mx_h[...], mx_l[...]), NN)
    strips = [pl.ds(k * half * chunk, half * chunk) for k in range(2)]
    for k in range(2):
        turned[rows_of[k], :] = ahead[k].get().T
        for narrow, broad in main_corners(cores[k]):
            wide[broad] = turned[narrow]
        mixed = dot3(ty, halves(wide[:total_y, strips[k]]), NN)
        spectrum = spectrum + dot3(halves(mixed), (mx_h[strips[k], :], mx_l[strips[k], :]), NN)
    spectrum = halves(spectrum * weight[...])
    after = exchanges(back, home, 3)
    mixed = []
    for k in range(2):
        mixed.append(halves(dot3(spectrum, (mx_h[strips[k], :], mx_l[strips[k], :]), NT)))
        wide[:total_y, strips[k]] = dot3(ty, mixed[k], TN)
        for narrow, broad in main_corners(cores[k]):
            turned[narrow] = wide[broad]
        after[k].put(turned[rows_of[k], :].T)
    mixed.append(halves(dot3(spectrum, (mx_h[tails, :], mx_l[tails, :]), NT)))
    wide[:total_y, split:] = dot3(ty, mixed[2], TN)
    joined = tuple(jnp.concatenate(group, axis=1) for group in zip(*mixed))
    wide[total_y:, :] = dot3(ty_rim, joined, TN)
    turned[rows_of[2], :] = jnp.zeros((ROWS - CORE, NZ), jnp.float32)
    for narrow, broad in edge_corners():
        turned[narrow] = wide[broad]
    after[2].put(turned[rows_of[2], :].T)

    def fields(rows, span):
        def sampled_with(high, low):
            stacked = jnp.dot(
                window[: 2 * rows], high[:, span], preferred_element_type=jnp.float32
            )
            rest = jnp.dot(window[:rows], low[:, span], preferred_element_type=jnp.float32)
            return stacked[:rows] + (stacked[rows:] + rest)

        return sampled_with(rz_h, rz_l), sampled_with(dz_h, dz_l)

    def over_x(planes, rows, field):
        total = rows[planes[0] : planes[0] + 1] * field[0:CY]
        for k, x in enumerate(planes[1:], 1):
            total = total + rows[x : x + 1] * field[k * CY : (k + 1) * CY]
        return total

    def four_sums(planes, near, level, tilt):
        masks_x, masks_y = near.x(), near.y()
        row_x, tilt_x = pick(masks_x, near.values(0)), pick(masks_x, near.slopes(0))
        row_y, tilt_y = pick(masks_y, near.values(1)), pick(masks_y, near.slopes(1))
        plain = over_x(planes, row_x, level)
        return [
            jnp.sum(product, axis=0, keepdims=True)
            for product in (
                over_x(planes, tilt_x, level) * row_y,
                plain * tilt_y,
                over_x(planes, row_x, tilt) * row_y,
                plain * row_y,
            )
        ]

    def set_window(got):
        field = halves(dot3(halves(got.T), tz, NN))
        window[: 2 * got.shape[1]] = jnp.concatenate(field, axis=0)

    def gather_core(k, span, near, amount):
        sums = four_sums(cores[k], near, *fields(half * CY, span))
        for d in range(4):
            part[d, :, span] = sums[d] + part[d, :, span] if k else sums[d]

    for k in range(2):
        set_window(after[k].get())
        tiles(functools.partial(gather_core, k))

    def gather_edge(span, near, amount):
        level, tilt = fields(ROWS - CORE, span)
        sums = four_sums(range(CX, SPAN), near, level, tilt)
        masks_x, masks_y = near.rim()
        row_x, tilt_x = pick(masks_x, near.values(0)), pick(masks_x, near.slopes(0))
        row_y, tilt_y = pick(masks_y, near.values(1)), pick(masks_y, near.slopes(1))
        level, tilt = level[MAIN - CORE :], tilt[MAIN - CORE :]
        flat = row_x * row_y
        extra = (level * tilt_x * row_y, level * row_x * tilt_y, tilt * flat, level * flat)
        sums = [
            sums[d] + (jnp.sum(extra[d], axis=0, keepdims=True) + part[d, :, span])
            for d in range(4)
        ]
        for d in range(3):
            scale = jnp.full((1, TILE), spacing[d], jnp.float32)
            forces[d, :, span] = -amount * sums[d] / scale
        energy[:, span] = 0.5 * amount * sums[3]

    set_window(after[2].get())
    tiles(gather_edge)


def signed(length):
    index = np.arange(length)
    return np.where(2 * index < length, index, index - length)


def moduli(length):
    return 1.0 / ((2.0 + np.cos(2.0 * np.pi / length * np.arange(length))) / 3.0) ** 2


def middle_tables(pieces_x, pieces_y):
    pieces = pieces_x * pieces_y
    slice_z = NZ // pieces
    total_x, total_y = CX * pieces_x, CY * pieces_y
    rim = np.zeros((total_y, pieces_y, RIM))
    starts = CY * (np.arange(pieces_y) + 1)
    places = starts[:, None] + np.arange(RIM - 1)[None, :]
    rim[:, :, : RIM - 1] = cas(places.reshape(-1), total_y).reshape(total_y, pieces_y, RIM - 1)
    ty = np.concatenate([cas(np.arange(total_y), total_y), rim.reshape(total_y, -1)], axis=1)
    places = (np.arange(SPAN)[:, None] + CX * np.arange(pieces_x)[None, :]).reshape(-1)
    mx = np.kron(cas(places, total_x).T, np.eye(slice_z))
    depth = -(-mx.shape[0] // 128) * 128
    mx = np.concatenate([mx, np.zeros((depth - mx.shape[0], mx.shape[1]))], axis=0)
    row1 = np.repeat((signed(total_x) / total_x) ** 2, slice_z)[None, :]
    row3 = np.tile(((signed(NZ) / NZ) ** 2).reshape(pieces, slice_z), (1, total_x))
    rowm = np.tile(moduli(NZ).reshape(pieces, slice_z), (1, total_x))
    rowm = rowm * np.repeat(moduli(total_x), slice_z)[None, :]
    col2 = ((signed(total_y) / total_y) ** 2)[:, None]
    colm = moduli(total_y)[:, None]
    plain = tuple(jnp.asarray(t, jnp.float32) for t in (row1, row3, rowm, col2, colm))
    return constant_halves(ty) + constant_halves(mx) + plain


def local(base_cell, cell_offset, charges, spacing, ewald_beta):
    pieces_x = lax.axis_size("px")
    pieces_y = lax.axis_size("py")
    pieces = pieces_x * pieces_y
    charge = charges.reshape(1, -1)
    atoms = charge.shape[1]
    cells = jnp.transpose(base_cell, (0, 3, 1, 2)).reshape(3, 1, atoms)
    offs = jnp.transpose(cell_offset, (0, 3, 1, 2)).reshape(3, 1, atoms)
    tz = constant_halves(cas(np.arange(NZ), NZ))
    tables = middle_tables(pieces_x, pieces_y)
    vmem = pl.BlockSpec(memory_space=pltpu.VMEM)
    scalars = pl.BlockSpec(memory_space=pltpu.SMEM)
    anywhere = pl.BlockSpec(memory_space=pl.ANY)
    blocks = pltpu.VMEM((pieces, NZ // pieces, ROWS), jnp.float32)
    profile = pltpu.VMEM((NZ, atoms), jnp.bfloat16)
    forces, energy = pl.pallas_call(
        functools.partial(kernel, pieces_x, pieces_y),
        out_shape=(
            jax.ShapeDtypeStruct((3, 1, atoms), jnp.float32),
            jax.ShapeDtypeStruct((1, atoms), jnp.float32),
        ),
        in_specs=[vmem] * 3 + [scalars] * 2 + [vmem] * 4 + [anywhere] * 2 + [vmem] * 5,
        out_specs=(vmem, vmem),
        scratch_shapes=[
            pltpu.VMEM((ROWS, NZ), jnp.float32),
            pltpu.VMEM((tables[0].shape[1], tables[2].shape[0]), jnp.float32),
            pltpu.VMEM(tables[2].shape, jnp.bfloat16),
            pltpu.VMEM(tables[2].shape, jnp.bfloat16),
            profile,
            profile,
            profile,
            profile,
            pltpu.VMEM((CORE, NZ), jnp.bfloat16),
            pltpu.VMEM((4, 1, atoms), jnp.float32),
            pltpu.VMEM((tables[0].shape[0], tables[2].shape[1]), jnp.float32),
            blocks,
            blocks,
            blocks,
            blocks,
            pltpu.SemaphoreType.DMA((2,)),
            pltpu.SemaphoreType.DMA((6, pieces)),
            pltpu.SemaphoreType.DMA((6, pieces)),
        ],
        compiler_params=pltpu.CompilerParams(
            vmem_limit_bytes=VMEM_LIMIT, collective_id=0, has_side_effects=True
        ),
        name="ewald",
    )(cells, offs, charge, spacing, ewald_beta, *tz, *tables)
    forces = jnp.transpose(forces.reshape(1, 3, 1, atoms), (0, 2, 3, 1))
    return forces, energy.reshape(charges.shape)


def solution(mesh):
    placed = (P("px", "py", None, None), P("px", "py", None, None), P("px", "py", None), P(), P())
    return jax.shard_map(
        local,
        mesh=mesh,
        in_specs=placed,
        out_specs=(P("px", "py", None, None), P("px", "py", None)),
        check_vma=False,
    )
```

```python
import functools

import jax
import jax.numpy as jnp
import numpy as np
from jax import lax
from jax.experimental import pallas as pl
from jax.experimental.pallas import tpu as pltpu
from jax.sharding import PartitionSpec as P

CX = 16
CY = 16
NZ = 256
SPAN = CX + 3
RIM = 4
MAIN = SPAN * CY
CORE = CX * CY
ROWS = -(-(MAIN + SPAN * RIM) // 128) * 128
TILE = 512
VMEM_LIMIT = 60 * 1024 * 1024
NN = (((1,), (0,)), ((), ()))
NT = (((1,), (1,)), ((), ()))
TN = (((0,), (0,)), ((), ()))


def cas(positions, length):
    angles = 2.0 * np.pi / length * (np.outer(np.arange(length), positions) % length)
    return np.cos(angles) + np.sin(angles)


def halves(value):
    high = value.astype(jnp.bfloat16)
    return high, (value - high.astype(jnp.float32)).astype(jnp.bfloat16)


def constant_halves(table):
    table = np.asarray(table, np.float32)
    high = table.astype(jnp.bfloat16)
    return jnp.asarray(high), jnp.asarray((table - high.astype(np.float32)).astype(jnp.bfloat16))


def dot3(left, right, dims):
    def product(a, b):
        return lax.dot_general(a, b, dims, preferred_element_type=jnp.float32)

    if dims == TN:
        cross = product(left[0], right[1]) + product(left[1], right[0])
        return product(left[0], right[0]) + cross
    rows = left[0].shape[0]
    stacked = product(jnp.concatenate(left, axis=0), right[0])
    return stacked[:rows] + (stacked[rows:] + product(left[0], right[1]))


def spline_values(t):
    rest = 1.0 - t
    square = t * t
    cube = square * t
    return (
        rest * rest * rest / 6.0,
        (3.0 * cube - 6.0 * square + 4.0) / 6.0,
        (-3.0 * cube + 3.0 * square + 3.0 * t + 1.0) / 6.0,
        cube / 6.0,
    )


def spline_slopes(t):
    rest = 1.0 - t
    square = t * t
    return (-0.5 * rest * rest, 1.5 * square - 2.0 * t, -1.5 * square + t + 0.5, 0.5 * square)


def pick(masks, weights):
    chosen = jnp.where(masks[3], weights[3], 0.0)
    for step in (2, 1, 0):
        chosen = jnp.where(masks[step], weights[step], chosen)
    return chosen


def masks_of(slots, start):
    steps = slots - start
    return [steps == step for step in range(4)]


def rows_iota(rows, width):
    return lax.broadcasted_iota(jnp.int32, (rows, width), 0)


class Stencil:
    def __init__(self, cells, offs, span):
        self.near_x = cells[0, :, span] - lax.axis_index("px") * CX
        self.near_y = cells[1, :, span] - lax.axis_index("py") * CY
        self.near_z = cells[2, :, span]
        self.width = self.near_x.shape[1]
        self.t = [offs[d, :, span] for d in range(3)]

    def x(self):
        return masks_of(rows_iota(24, self.width), self.near_x)

    def y(self):
        return masks_of(rows_iota(CY, self.width), self.near_y)

    def rim(self):
        rim = rows_iota(ROWS - MAIN, self.width)
        return masks_of(rim // RIM, self.near_x), masks_of(CY + rim % RIM, self.near_y)

    def z(self):
        steps = (rows_iota(NZ, self.width) - self.near_z) & (NZ - 1)
        return [steps == step for step in range(4)]

    def values(self, d):
        return spline_values(self.t[d])

    def slopes(self, d):
        return spline_slopes(self.t[d])


class Exchange:
    def __init__(self, pieces_x, src, dst, lanes, send_sem, recv_sem):
        self.pieces_x, self.src, self.dst, self.lanes = pieces_x, src, dst, lanes
        self.send_sem, self.recv_sem = send_sem, recv_sem
        self.pieces = src.shape[0]
        self.mine = lax.axis_index("py") * pieces_x + lax.axis_index("px")

    def copy(self, step, here, there):
        peer = (self.mine + step) % self.pieces
        return pltpu.make_async_remote_copy(
            src_ref=self.src.at[peer if here is None else here, :, self.lanes],
            dst_ref=self.dst.at[there, :, self.lanes],
            send_sem=self.send_sem,
            recv_sem=self.recv_sem,
            device_id=(peer % self.pieces_x, peer // self.pieces_x),
            device_id_type=pl.DeviceIdType.MESH,
        )

    def put(self, value):
        self.src[:, :, self.lanes] = value.reshape(self.src.shape[:2] + (value.shape[1],))

        for step in range(1, self.pieces):
            self.copy(step, None, self.mine).start()

        self.dst[self.mine, :, self.lanes] = self.src[self.mine, :, self.lanes]

    def get(self):
        every = pl.ds(0, self.pieces - 1)
        self.copy(1, every, every).wait()
        return self.dst[:, :, self.lanes].reshape(NZ, -1)


def kernel(
    pieces_x, pieces_y, cells, offs, charge, spacing, beta, tz_h, tz_l, ty_h, ty_l, mx_hbm_h,
    mx_hbm_l, row1, row3, rowm, col2, colm, forces, energy, grid, wide, mx_h, mx_l, rz_h, rz_l,
    dz_h, dz_l, window, part, weight, src, dst, back, home, table_sem, send_sem, recv_sem,
):
    pieces = pieces_x * pieces_y
    slice_z = NZ // pieces
    mine = lax.axis_index("py") * pieces_x + lax.axis_index("px")
    core, edge = pl.ds(0, CORE), pl.ds(CORE, ROWS - CORE)
    loads = [
        pltpu.make_async_copy(mx_hbm_h, mx_h, table_sem.at[0]),
        pltpu.make_async_copy(mx_hbm_l, mx_l, table_sem.at[1]),
    ]
    for load in loads:
        load.start()
    barrier = pltpu.get_barrier_semaphore()

    @pl.loop(1, pieces)
    def _(step):
        peer = (mine + step) % pieces
        pl.semaphore_signal(
            barrier,
            inc=1,
            device_id=(peer % pieces_x, peer // pieces_x),
            device_id_type=pl.DeviceIdType.MESH,
        )

    def tiles(body):
        @pl.loop(0, charge.shape[1] // TILE)
        def _(step):
            span = pl.ds(pl.multiple_of(step * TILE, TILE), TILE)
            body(span, Stencil(cells, offs, span), charge[:, span])

    tz = (tz_h[...], tz_l[...])
    grid[...] = jnp.zeros_like(grid)

    def spread_core(span, near, amount):
        row_x = pick(near.x(), [w * amount for w in near.values(0)])
        row_y = pick(near.y(), near.values(1))
        planes = jnp.concatenate([row_x[x : x + 1] * row_y for x in range(CX)], axis=0)
        profile = halves(pick(near.z(), near.values(2)))
        rz_h[:, span], rz_l[:, span] = profile
        grid[core, :] += dot3(halves(planes), profile, NT)

    tiles(spread_core)
    ahead = [
        Exchange(pieces_x, src, dst, lanes, send_sem.at[k], recv_sem.at[k])
        for k, lanes in enumerate((core, edge))
    ]
    value = dot3(tz, halves(grid[core, :]), NT)
    pl.semaphore_wait(barrier, pieces - 1)
    ahead[0].put(value)

    def spread_edge(span, near, amount):
        heavy = [w * amount for w in near.values(0)]
        row_x = pick(near.x(), heavy)
        row_y = pick(near.y(), near.values(1))
        rim_x, rim_y = near.rim()
        rim = pick(rim_x, heavy) * pick(rim_y, near.values(1))
        planes = [row_x[x : x + 1] * row_y for x in range(CX, SPAN)] + [rim]
        planes = jnp.concatenate(planes, axis=0)
        grid[edge, :] += dot3(halves(planes), (rz_h[:, span], rz_l[:, span]), NT)

    tiles(spread_edge)
    ahead[1].put(dot3(tz, halves(grid[edge, :]), NT))

    def slopes_z(span, near, amount):
        dz_h[:, span], dz_l[:, span] = halves(pick(near.z(), near.slopes(2)))

    tiles(slopes_z)

    chunk = pieces_x * slice_z
    total_x = CX * pieces_x
    total_y = CY * pieces_y
    split = CX * chunk
    turned = grid

    def main_corners(planes):
        for x in planes:
            for j in range(pieces_y):
                lanes, own = pl.ds(x * chunk, chunk), pl.ds(j * chunk, chunk)
                yield (pl.ds(x * CY, CY), own), (pl.ds(j * CY, CY), lanes)

    def rim_corners():
        for x in range(SPAN):
            for j in range(pieces_y):
                lanes, own = pl.ds(x * chunk, chunk), pl.ds(j * chunk, chunk)
                yield (pl.ds(MAIN + x * RIM, RIM), own), (pl.ds(total_y + j * RIM, RIM), lanes)

    def edge_corners():
        yield from main_corners(range(CX, SPAN))
        yield from rim_corners()

    tails = pl.ds(split, wide.shape[1] - split)
    wide[:, tails] = jnp.zeros((wide.shape[0], wide.shape[1] - split), jnp.float32)
    ty = (ty_h[:, :total_y], ty_l[:, :total_y])
    ty_rim = (ty_h[:, total_y:], ty_l[:, total_y:])
    width = mx_h.shape[1]

    def spread_scalar(ref, place):
        return jnp.full((1, width), ref[place], jnp.float32)

    s0, s1, s2 = (spread_scalar(spacing, d) for d in range(3))
    b = spread_scalar(beta, 0)
    squares = row1[...] / (s0 * s0) + row3[pl.ds(mine, 1), :] / (s2 * s2)
    squares = squares + col2[...] * (1.0 / (s1 * s1))
    safe = jnp.where(squares > 0.0, squares, 1.0)
    volume = s0 * s1 * s2 * float(total_x * total_y * NZ)
    table = jnp.exp(safe * (-(np.pi**2) / (b * b))) / (safe * (np.pi * volume))
    table = table * (rowm[pl.ds(mine, 1), :] * colm[...])
    weight[...] = jnp.where(squares > 0.0, table, 0.0)
    for load in loads:
        load.wait()
    turned[core, :] = ahead[0].get().T
    for narrow, broad in main_corners(range(CX)):
        wide[broad] = turned[narrow]
    first = dot3(ty, halves(wide[:total_y, :split]), NN)
    turned[edge, :] = ahead[1].get().T
    for narrow, broad in edge_corners():
        wide[broad] = turned[narrow]
    last = dot3(ty, halves(wide[:total_y, split:]), NN)
    mixed = jnp.concatenate([first, last], axis=1) + dot3(ty_rim, halves(wide[total_y:, :]), NN)
    mx = (mx_h[...], mx_l[...])
    spectrum = dot3(halves(mixed), mx, NN)
    spectrum = spectrum * weight[...]
    mixed = halves(dot3(halves(spectrum), mx, NT))
    after = [
        Exchange(pieces_x, back, home, lanes, send_sem.at[2 + k], recv_sem.at[2 + k])
        for k, lanes in enumerate((core, edge))
    ]
    wide[total_y:, :] = dot3(ty_rim, mixed, TN)
    wide[:total_y, split:] = dot3(ty, tuple(half[:, split:] for half in mixed), TN)
    turned[edge, :] = jnp.zeros((ROWS - CORE, NZ), jnp.float32)
    for narrow, broad in edge_corners():
        turned[narrow] = wide[broad]
    after[1].put(turned[edge, :].T)
    wide[:total_y, :split] = dot3(ty, tuple(half[:, :split] for half in mixed), TN)
    for narrow, broad in main_corners(range(CX)):
        turned[narrow] = wide[broad]
    after[0].put(turned[core, :].T)

    def fields(rows, span):
        def sampled_with(high, low):
            stacked = jnp.dot(
                window[: 2 * rows], high[:, span], preferred_element_type=jnp.float32
            )
            rest = jnp.dot(window[:rows], low[:, span], preferred_element_type=jnp.float32)
            return stacked[:rows] + (stacked[rows:] + rest)

        return sampled_with(rz_h, rz_l), sampled_with(dz_h, dz_l)

    def over_x(planes, rows, field):
        total = rows[planes[0] : planes[0] + 1] * field[0:CY]
        for k, x in enumerate(planes[1:], 1):
            total = total + rows[x : x + 1] * field[k * CY : (k + 1) * CY]
        return total

    def four_sums(planes, near, level, tilt):
        masks_x, masks_y = near.x(), near.y()
        row_x, tilt_x = pick(masks_x, near.values(0)), pick(masks_x, near.slopes(0))
        row_y, tilt_y = pick(masks_y, near.values(1)), pick(masks_y, near.slopes(1))
        plain = over_x(planes, row_x, level)
        return [
            jnp.sum(product, axis=0, keepdims=True)
            for product in (
                over_x(planes, tilt_x, level) * row_y,
                plain * tilt_y,
                over_x(planes, row_x, tilt) * row_y,
                plain * row_y,
            )
        ]

    def set_window(got):
        field = halves(dot3(halves(got.T), tz, NN))
        window[: 2 * got.shape[1]] = jnp.concatenate(field, axis=0)

    def gather_edge(span, near, amount):
        level, tilt = fields(ROWS - CORE, span)
        sums = four_sums(range(CX, SPAN), near, level, tilt)
        masks_x, masks_y = near.rim()
        row_x, tilt_x = pick(masks_x, near.values(0)), pick(masks_x, near.slopes(0))
        row_y, tilt_y = pick(masks_y, near.values(1)), pick(masks_y, near.slopes(1))
        level, tilt = level[MAIN - CORE :], tilt[MAIN - CORE :]
        flat = row_x * row_y
        extra = (level * tilt_x * row_y, level * row_x * tilt_y, tilt * flat, level * flat)
        for d in range(4):
            part[d, :, span] = sums[d] + jnp.sum(extra[d], axis=0, keepdims=True)

    set_window(after[1].get())
    tiles(gather_edge)

    def gather_core(span, near, amount):
        sums = four_sums(range(CX), near, *fields(CORE, span))
        for d in range(3):
            scale = jnp.full((1, TILE), spacing[d], jnp.float32)
            forces[d, :, span] = -amount * (sums[d] + part[d, :, span]) / scale
        energy[:, span] = 0.5 * amount * (sums[3] + part[3, :, span])

    set_window(after[0].get())
    tiles(gather_core)


def signed(length):
    index = np.arange(length)
    return np.where(2 * index < length, index, index - length)


def moduli(length):
    return 1.0 / ((2.0 + np.cos(2.0 * np.pi / length * np.arange(length))) / 3.0) ** 2


def middle_tables(pieces_x, pieces_y):
    pieces = pieces_x * pieces_y
    slice_z = NZ // pieces
    total_x, total_y = CX * pieces_x, CY * pieces_y
    rim = np.zeros((total_y, pieces_y, RIM))
    starts = CY * (np.arange(pieces_y) + 1)
    places = starts[:, None] + np.arange(RIM - 1)[None, :]
    rim[:, :, : RIM - 1] = cas(places.reshape(-1), total_y).reshape(total_y, pieces_y, RIM - 1)
    ty = np.concatenate([cas(np.arange(total_y), total_y), rim.reshape(total_y, -1)], axis=1)
    places = (np.arange(SPAN)[:, None] + CX * np.arange(pieces_x)[None, :]).reshape(-1)
    mx = np.kron(cas(places, total_x).T, np.eye(slice_z))
    depth = -(-mx.shape[0] // 128) * 128
    mx = np.concatenate([mx, np.zeros((depth - mx.shape[0], mx.shape[1]))], axis=0)
    row1 = np.repeat((signed(total_x) / total_x) ** 2, slice_z)[None, :]
    row3 = np.tile(((signed(NZ) / NZ) ** 2).reshape(pieces, slice_z), (1, total_x))
    rowm = np.tile(moduli(NZ).reshape(pieces, slice_z), (1, total_x))
    rowm = rowm * np.repeat(moduli(total_x), slice_z)[None, :]
    col2 = ((signed(total_y) / total_y) ** 2)[:, None]
    colm = moduli(total_y)[:, None]
    plain = tuple(jnp.asarray(t, jnp.float32) for t in (row1, row3, rowm, col2, colm))
    return constant_halves(ty) + constant_halves(mx) + plain


def local(base_cell, cell_offset, charges, spacing, ewald_beta):
    pieces_x = lax.axis_size("px")
    pieces_y = lax.axis_size("py")
    pieces = pieces_x * pieces_y
    charge = charges.reshape(1, -1)
    atoms = charge.shape[1]
    cells = jnp.transpose(base_cell, (0, 3, 1, 2)).reshape(3, 1, atoms)
    offs = jnp.transpose(cell_offset, (0, 3, 1, 2)).reshape(3, 1, atoms)
    tz = constant_halves(cas(np.arange(NZ), NZ))
    tables = middle_tables(pieces_x, pieces_y)
    vmem = pl.BlockSpec(memory_space=pltpu.VMEM)
    scalars = pl.BlockSpec(memory_space=pltpu.SMEM)
    anywhere = pl.BlockSpec(memory_space=pl.ANY)
    blocks = pltpu.VMEM((pieces, NZ // pieces, ROWS), jnp.float32)
    profile = pltpu.VMEM((NZ, atoms), jnp.bfloat16)
    forces, energy = pl.pallas_call(
        functools.partial(kernel, pieces_x, pieces_y),
        out_shape=(
            jax.ShapeDtypeStruct((3, 1, atoms), jnp.float32),
            jax.ShapeDtypeStruct((1, atoms), jnp.float32),
        ),
        in_specs=[vmem] * 3 + [scalars] * 2 + [vmem] * 4 + [anywhere] * 2 + [vmem] * 5,
        out_specs=(vmem, vmem),
        scratch_shapes=[
            pltpu.VMEM((ROWS, NZ), jnp.float32),
            pltpu.VMEM((tables[0].shape[1], tables[2].shape[0]), jnp.float32),
            pltpu.VMEM(tables[2].shape, jnp.bfloat16),
            pltpu.VMEM(tables[2].shape, jnp.bfloat16),
            profile,
            profile,
            profile,
            profile,
            pltpu.VMEM((2 * CORE, NZ), jnp.bfloat16),
            pltpu.VMEM((4, 1, atoms), jnp.float32),
            pltpu.VMEM((tables[0].shape[0], tables[2].shape[1]), jnp.float32),
            blocks,
            blocks,
            blocks,
            blocks,
            pltpu.SemaphoreType.DMA((2,)),
            pltpu.SemaphoreType.DMA((4,)),
            pltpu.SemaphoreType.DMA((4,)),
        ],
        compiler_params=pltpu.CompilerParams(
            vmem_limit_bytes=VMEM_LIMIT, collective_id=0, has_side_effects=True
        ),
        name="ewald",
    )(cells, offs, charge, spacing, ewald_beta, *tz, *tables)
    forces = jnp.transpose(forces.reshape(1, 3, 1, atoms), (0, 2, 3, 1))
    return forces, energy.reshape(charges.shape)


def solution(mesh):
    placed = (P("px", "py", None, None), P("px", "py", None, None), P("px", "py", None), P(), P())
    return jax.shard_map(
        local,
        mesh=mesh,
        in_specs=placed,
        out_specs=(P("px", "py", None, None), P("px", "py", None)),
        check_vma=False,
    )
```

```python
import functools

import jax
import jax.numpy as jnp
import numpy as np
from jax import lax
from jax.experimental import pallas as pl
from jax.experimental.pallas import tpu as pltpu
from jax.sharding import PartitionSpec as P

CX = 16
CY = 16
NZ = 256
SPAN = CX + 3
RIM = 4
MAIN = SPAN * CY
CORE = CX * CY
ROWS = -(-(MAIN + SPAN * RIM) // 128) * 128
TILE = 512
TWIN = 2
VMEM_LIMIT = 60 * 1024 * 1024
NN = (((1,), (0,)), ((), ()))
NT = (((1,), (1,)), ((), ()))
TN = (((0,), (0,)), ((), ()))


def cas(positions, length):
    angles = 2.0 * np.pi / length * (np.outer(np.arange(length), positions) % length)
    return np.cos(angles) + np.sin(angles)


def halves(value):
    high = value.astype(jnp.bfloat16)
    return high, (value - high.astype(jnp.float32)).astype(jnp.bfloat16)


def constant_halves(table):
    table = np.asarray(table, np.float32)
    high = table.astype(jnp.bfloat16)
    return jnp.asarray(high), jnp.asarray((table - high.astype(np.float32)).astype(jnp.bfloat16))


def dot3(left, right, dims):
    def product(a, b):
        return lax.dot_general(a, b, dims, preferred_element_type=jnp.float32)

    if dims == TN:
        cross = product(left[0], right[1]) + product(left[1], right[0])
        return product(left[0], right[0]) + cross
    rows = left[0].shape[0]
    stacked = product(jnp.concatenate(left, axis=0), right[0])
    return stacked[:rows] + (stacked[rows:] + product(left[0], right[1]))


def spline_values(t):
    rest = 1.0 - t
    square = t * t
    cube = square * t
    return (
        rest * rest * rest / 6.0,
        (3.0 * cube - 6.0 * square + 4.0) / 6.0,
        (-3.0 * cube + 3.0 * square + 3.0 * t + 1.0) / 6.0,
        cube / 6.0,
    )


def spline_slopes(t):
    rest = 1.0 - t
    square = t * t
    return (-0.5 * rest * rest, 1.5 * square - 2.0 * t, -1.5 * square + t + 0.5, 0.5 * square)


def pick(masks, weights):
    chosen = jnp.where(masks[3], weights[3], 0.0)
    for step in (2, 1, 0):
        chosen = jnp.where(masks[step], weights[step], chosen)
    return chosen


def masks_of(slots, start):
    steps = slots - start
    return [steps == step for step in range(4)]


def rows_iota(rows, width):
    return lax.broadcasted_iota(jnp.int32, (rows, width), 0)


class Stencil:
    def __init__(self, cells, offs, span):
        self.near_x = cells[0, :, span] - lax.axis_index("px") * CX
        self.near_y = cells[1, :, span] - lax.axis_index("py") * CY
        self.near_z = cells[2, :, span]
        self.width = self.near_x.shape[1]
        self.t = [offs[d, :, span] for d in range(3)]

    def x(self):
        return masks_of(rows_iota(24, self.width), self.near_x)

    def y(self):
        return masks_of(rows_iota(CY, self.width), self.near_y)

    def rim(self):
        rim = rows_iota(ROWS - MAIN, self.width)
        return masks_of(rim // RIM, self.near_x), masks_of(CY + rim % RIM, self.near_y)

    def z(self):
        steps = (rows_iota(NZ, self.width) - self.near_z) & (NZ - 1)
        return [steps == step for step in range(4)]

    def values(self, d):
        return spline_values(self.t[d])

    def slopes(self, d):
        return spline_slopes(self.t[d])


class Exchange:
    def __init__(self, pieces_x, src, dst, lanes, send_sem, recv_sem):
        self.pieces_x, self.src, self.dst, self.lanes = pieces_x, src, dst, lanes
        self.send_sem, self.recv_sem = send_sem, recv_sem
        self.pieces = src.shape[0]
        self.mine = lax.axis_index("py") * pieces_x + lax.axis_index("px")

    def copy(self, step, here, there):
        peer = (self.mine + step) % self.pieces
        return pltpu.make_async_remote_copy(
            src_ref=self.src.at[peer if here is None else here, :, self.lanes],
            dst_ref=self.dst.at[there, :, self.lanes],
            send_sem=self.send_sem,
            recv_sem=self.recv_sem,
            device_id=(peer % self.pieces_x, peer // self.pieces_x),
            device_id_type=pl.DeviceIdType.MESH,
        )

    def put(self, value):
        self.src[:, :, self.lanes] = value.reshape(self.src.shape[:2] + (value.shape[1],))

        for step in range(1, self.pieces):
            self.copy(step, None, self.mine).start()

        self.dst[self.mine, :, self.lanes] = self.src[self.mine, :, self.lanes]

    def get(self):
        every = pl.ds(0, self.pieces - 1)
        self.copy(1, every, every).wait()
        return self.dst[:, :, self.lanes].reshape(NZ, -1)


def kernel(
    pieces_x, pieces_y, cells, offs, charge, spacing, beta, tz_h, tz_l, ty_h, ty_l, mx_hbm_h,
    mx_hbm_l, row1, row3, rowm, col2, colm, forces, energy, grid, wide, mx_h, mx_l, rz_h, rz_l,
    dz_h, dz_l, window, part, weight, src, dst, back, home, table_sem, send_sem, recv_sem,
):
    pieces = pieces_x * pieces_y
    slice_z = NZ // pieces
    mine = lax.axis_index("py") * pieces_x + lax.axis_index("px")
    core, edge = pl.ds(0, CORE), pl.ds(CORE, ROWS - CORE)
    loads = [
        pltpu.make_async_copy(mx_hbm_h, mx_h, table_sem.at[0]),
        pltpu.make_async_copy(mx_hbm_l, mx_l, table_sem.at[1]),
    ]
    for load in loads:
        load.start()
    barrier = pltpu.get_barrier_semaphore()

    for step in range(1, pieces):
        peer = (mine + step) % pieces
        pl.semaphore_signal(
            barrier,
            inc=1,
            device_id=(peer % pieces_x, peer // pieces_x),
            device_id_type=pl.DeviceIdType.MESH,
        )

    def tiles(body):
        @pl.loop(0, charge.shape[1] // (TILE * TWIN))
        def _(step):
            for twin in range(TWIN):
                span = pl.ds(pl.multiple_of((step * TWIN + twin) * TILE, TILE), TILE)
                body(span, Stencil(cells, offs, span), charge[:, span])

    tz = (tz_h[...], tz_l[...])
    grid[...] = jnp.zeros_like(grid)

    def spread_core(span, near, amount):
        row_x = pick(near.x(), [w * amount for w in near.values(0)])
        row_y = pick(near.y(), near.values(1))
        planes = jnp.concatenate([row_x[x : x + 1] * row_y for x in range(CX)], axis=0)
        profile = halves(pick(near.z(), near.values(2)))
        rz_h[:, span], rz_l[:, span] = profile
        grid[core, :] += dot3(halves(planes), profile, NT)

    tiles(spread_core)
    ahead = [
        Exchange(pieces_x, src, dst, lanes, send_sem.at[k], recv_sem.at[k])
        for k, lanes in enumerate((core, edge))
    ]
    value = dot3(tz, halves(grid[core, :]), NT)
    pl.semaphore_wait(barrier, pieces - 1)
    ahead[0].put(value)

    def spread_edge(span, near, amount):
        heavy = [w * amount for w in near.values(0)]
        row_x = pick(near.x(), heavy)
        row_y = pick(near.y(), near.values(1))
        rim_x, rim_y = near.rim()
        rim = pick(rim_x, heavy) * pick(rim_y, near.values(1))
        planes = [row_x[x : x + 1] * row_y for x in range(CX, SPAN)] + [rim]
        planes = jnp.concatenate(planes, axis=0)
        grid[edge, :] += dot3(halves(planes), (rz_h[:, span], rz_l[:, span]), NT)

    tiles(spread_edge)
    ahead[1].put(dot3(tz, halves(grid[edge, :]), NT))

    def slopes_z(span, near, amount):
        dz_h[:, span], dz_l[:, span] = halves(pick(near.z(), near.slopes(2)))

    tiles(slopes_z)

    chunk = pieces_x * slice_z
    total_x = CX * pieces_x
    total_y = CY * pieces_y
    split = CX * chunk
    turned = grid

    def main_corners(planes):
        for x in planes:
            for j in range(pieces_y):
                lanes, own = pl.ds(x * chunk, chunk), pl.ds(j * chunk, chunk)
                yield (pl.ds(x * CY, CY), own), (pl.ds(j * CY, CY), lanes)

    def rim_corners():
        for x in range(SPAN):
            for j in range(pieces_y):
                lanes, own = pl.ds(x * chunk, chunk), pl.ds(j * chunk, chunk)
                yield (pl.ds(MAIN + x * RIM, RIM), own), (pl.ds(total_y + j * RIM, RIM), lanes)

    def edge_corners():
        yield from main_corners(range(CX, SPAN))
        yield from rim_corners()

    tails = pl.ds(split, wide.shape[1] - split)
    wide[:, tails] = jnp.zeros((wide.shape[0], wide.shape[1] - split), jnp.float32)
    ty = (ty_h[:, :total_y], ty_l[:, :total_y])
    ty_rim = (ty_h[:, total_y:], ty_l[:, total_y:])
    width = mx_h.shape[1]

    def spread_scalar(ref, place):
        return jnp.full((1, width), ref[place], jnp.float32)

    s0, s1, s2 = (spread_scalar(spacing, d) for d in range(3))
    b = spread_scalar(beta, 0)
    squares = row1[...] / (s0 * s0) + row3[pl.ds(mine, 1), :] / (s2 * s2)
    squares = squares + col2[...] * (1.0 / (s1 * s1))
    safe = jnp.where(squares > 0.0, squares, 1.0)
    volume = s0 * s1 * s2 * float(total_x * total_y * NZ)
    table = jnp.exp(safe * (-(np.pi**2) / (b * b))) / (safe * (np.pi * volume))
    table = table * (rowm[pl.ds(mine, 1), :] * colm[...])
    weight[...] = jnp.where(squares > 0.0, table, 0.0)
    for load in loads:
        load.wait()
    turned[core, :] = ahead[0].get().T
    for narrow, broad in main_corners(range(CX)):
        wide[broad] = turned[narrow]
    first = dot3(ty, halves(wide[:total_y, :split]), NN)
    turned[edge, :] = ahead[1].get().T
    for narrow, broad in edge_corners():
        wide[broad] = turned[narrow]
    last = dot3(ty, halves(wide[:total_y, split:]), NN)
    mixed = jnp.concatenate([first, last], axis=1) + dot3(ty_rim, halves(wide[total_y:, :]), NN)
    mx = (mx_h[...], mx_l[...])
    spectrum = dot3(halves(mixed), mx, NN)
    spectrum = spectrum * weight[...]
    mixed = halves(dot3(halves(spectrum), mx, NT))
    after = [
        Exchange(pieces_x, back, home, lanes, send_sem.at[2 + k], recv_sem.at[2 + k])
        for k, lanes in enumerate((core, edge))
    ]
    wide[total_y:, :] = dot3(ty_rim, mixed, TN)
    wide[:total_y, split:] = dot3(ty, tuple(half[:, split:] for half in mixed), TN)
    turned[edge, :] = jnp.zeros((ROWS - CORE, NZ), jnp.float32)
    for narrow, broad in edge_corners():
        turned[narrow] = wide[broad]
    after[1].put(turned[edge, :].T)
    wide[:total_y, :split] = dot3(ty, tuple(half[:, :split] for half in mixed), TN)
    for narrow, broad in main_corners(range(CX)):
        turned[narrow] = wide[broad]
    after[0].put(turned[core, :].T)

    def fields(rows, span):
        def sampled_with(high, low):
            stacked = jnp.dot(
                window[: 2 * rows], high[:, span], preferred_element_type=jnp.float32
            )
            rest = jnp.dot(window[:rows], low[:, span], preferred_element_type=jnp.float32)
            return stacked[:rows] + (stacked[rows:] + rest)

        return sampled_with(rz_h, rz_l), sampled_with(dz_h, dz_l)

    def over_x(planes, rows, field):
        total = rows[planes[0] : planes[0] + 1] * field[0:CY]
        for k, x in enumerate(planes[1:], 1):
            total = total + rows[x : x + 1] * field[k * CY : (k + 1) * CY]
        return total

    def four_sums(planes, near, level, tilt):
        masks_x, masks_y = near.x(), near.y()
        row_x, tilt_x = pick(masks_x, near.values(0)), pick(masks_x, near.slopes(0))
        row_y, tilt_y = pick(masks_y, near.values(1)), pick(masks_y, near.slopes(1))
        plain = over_x(planes, row_x, level)
        return [
            jnp.sum(product, axis=0, keepdims=True)
            for product in (
                over_x(planes, tilt_x, level) * row_y,
                plain * tilt_y,
                over_x(planes, row_x, tilt) * row_y,
                plain * row_y,
            )
        ]

    def set_window(got):
        field = halves(dot3(halves(got.T), tz, NN))
        window[: 2 * got.shape[1]] = jnp.concatenate(field, axis=0)

    def gather_edge(span, near, amount):
        level, tilt = fields(ROWS - CORE, span)
        sums = four_sums(range(CX, SPAN), near, level, tilt)
        masks_x, masks_y = near.rim()
        row_x, tilt_x = pick(masks_x, near.values(0)), pick(masks_x, near.slopes(0))
        row_y, tilt_y = pick(masks_y, near.values(1)), pick(masks_y, near.slopes(1))
        level, tilt = level[MAIN - CORE :], tilt[MAIN - CORE :]
        flat = row_x * row_y
        extra = (level * tilt_x * row_y, level * row_x * tilt_y, tilt * flat, level * flat)
        for d in range(4):
            part[d, :, span] = sums[d] + jnp.sum(extra[d], axis=0, keepdims=True)

    set_window(after[1].get())
    tiles(gather_edge)

    def gather_core(span, near, amount):
        sums = four_sums(range(CX), near, *fields(CORE, span))
        for d in range(3):
            scale = jnp.full((1, TILE), spacing[d], jnp.float32)
            forces[d, :, span] = -amount * (sums[d] + part[d, :, span]) / scale
        energy[:, span] = 0.5 * amount * (sums[3] + part[3, :, span])

    set_window(after[0].get())
    tiles(gather_core)


def signed(length):
    index = np.arange(length)
    return np.where(2 * index < length, index, index - length)


def moduli(length):
    return 1.0 / ((2.0 + np.cos(2.0 * np.pi / length * np.arange(length))) / 3.0) ** 2


def middle_tables(pieces_x, pieces_y):
    pieces = pieces_x * pieces_y
    slice_z = NZ // pieces
    total_x, total_y = CX * pieces_x, CY * pieces_y
    rim = np.zeros((total_y, pieces_y, RIM))
    starts = CY * (np.arange(pieces_y) + 1)
    places = starts[:, None] + np.arange(RIM - 1)[None, :]
    rim[:, :, : RIM - 1] = cas(places.reshape(-1), total_y).reshape(total_y, pieces_y, RIM - 1)
    ty = np.concatenate([cas(np.arange(total_y), total_y), rim.reshape(total_y, -1)], axis=1)
    places = (np.arange(SPAN)[:, None] + CX * np.arange(pieces_x)[None, :]).reshape(-1)
    mx = np.kron(cas(places, total_x).T, np.eye(slice_z))
    depth = -(-mx.shape[0] // 128) * 128
    mx = np.concatenate([mx, np.zeros((depth - mx.shape[0], mx.shape[1]))], axis=0)
    row1 = np.repeat((signed(total_x) / total_x) ** 2, slice_z)[None, :]
    row3 = np.tile(((signed(NZ) / NZ) ** 2).reshape(pieces, slice_z), (1, total_x))
    rowm = np.tile(moduli(NZ).reshape(pieces, slice_z), (1, total_x))
    rowm = rowm * np.repeat(moduli(total_x), slice_z)[None, :]
    col2 = ((signed(total_y) / total_y) ** 2)[:, None]
    colm = moduli(total_y)[:, None]
    plain = tuple(jnp.asarray(t, jnp.float32) for t in (row1, row3, rowm, col2, colm))
    return constant_halves(ty) + constant_halves(mx) + plain


def local(base_cell, cell_offset, charges, spacing, ewald_beta):
    pieces_x = lax.axis_size("px")
    pieces_y = lax.axis_size("py")
    pieces = pieces_x * pieces_y
    charge = charges.reshape(1, -1)
    atoms = charge.shape[1]
    cells = jnp.transpose(base_cell, (0, 3, 1, 2)).reshape(3, 1, atoms)
    offs = jnp.transpose(cell_offset, (0, 3, 1, 2)).reshape(3, 1, atoms)
    tz = constant_halves(cas(np.arange(NZ), NZ))
    tables = middle_tables(pieces_x, pieces_y)
    vmem = pl.BlockSpec(memory_space=pltpu.VMEM)
    scalars = pl.BlockSpec(memory_space=pltpu.SMEM)
    anywhere = pl.BlockSpec(memory_space=pl.ANY)
    blocks = pltpu.VMEM((pieces, NZ // pieces, ROWS), jnp.float32)
    profile = pltpu.VMEM((NZ, atoms), jnp.bfloat16)
    forces, energy = pl.pallas_call(
        functools.partial(kernel, pieces_x, pieces_y),
        out_shape=(
            jax.ShapeDtypeStruct((3, 1, atoms), jnp.float32),
            jax.ShapeDtypeStruct((1, atoms), jnp.float32),
        ),
        in_specs=[vmem] * 3 + [scalars] * 2 + [vmem] * 4 + [anywhere] * 2 + [vmem] * 5,
        out_specs=(vmem, vmem),
        scratch_shapes=[
            pltpu.VMEM((ROWS, NZ), jnp.float32),
            pltpu.VMEM((tables[0].shape[1], tables[2].shape[0]), jnp.float32),
            pltpu.VMEM(tables[2].shape, jnp.bfloat16),
            pltpu.VMEM(tables[2].shape, jnp.bfloat16),
            profile,
            profile,
            profile,
            profile,
            pltpu.VMEM((2 * CORE, NZ), jnp.bfloat16),
            pltpu.VMEM((4, 1, atoms), jnp.float32),
            pltpu.VMEM((tables[0].shape[0], tables[2].shape[1]), jnp.float32),
            blocks,
            blocks,
            blocks,
            blocks,
            pltpu.SemaphoreType.DMA((2,)),
            pltpu.SemaphoreType.DMA((4,)),
            pltpu.SemaphoreType.DMA((4,)),
        ],
        compiler_params=pltpu.CompilerParams(
            vmem_limit_bytes=VMEM_LIMIT, collective_id=0, has_side_effects=True
        ),
        name="ewald",
    )(cells, offs, charge, spacing, ewald_beta, *tz, *tables)
    forces = jnp.transpose(forces.reshape(1, 3, 1, atoms), (0, 2, 3, 1))
    return forces, energy.reshape(charges.shape)


def solution(mesh):
    placed = (P("px", "py", None, None), P("px", "py", None, None), P("px", "py", None), P(), P())
    return jax.shard_map(
        local,
        mesh=mesh,
        in_specs=placed,
        out_specs=(P("px", "py", None, None), P("px", "py", None)),
        check_vma=False,
    )
```

```python
import functools

import jax
import jax.numpy as jnp
import numpy as np
from jax import lax
from jax.experimental import pallas as pl
from jax.experimental.pallas import tpu as pltpu
from jax.sharding import PartitionSpec as P

CX = 16
CY = 16
NZ = 256
SPAN = CX + 3
RIM = 4
MAIN = SPAN * CY
CORE = CX * CY
ROWS = -(-(MAIN + SPAN * RIM) // 128) * 128
TILE = 512
TWIN = 4
VMEM_LIMIT = 60 * 1024 * 1024
NN = (((1,), (0,)), ((), ()))
NT = (((1,), (1,)), ((), ()))
TN = (((0,), (0,)), ((), ()))


def cas(positions, length):
    angles = 2.0 * np.pi / length * (np.outer(np.arange(length), positions) % length)
    return np.cos(angles) + np.sin(angles)


def halves(value):
    high = value.astype(jnp.bfloat16)
    return high, (value - high.astype(jnp.float32)).astype(jnp.bfloat16)


def constant_halves(table):
    table = np.asarray(table, np.float32)
    high = table.astype(jnp.bfloat16)
    return jnp.asarray(high), jnp.asarray((table - high.astype(np.float32)).astype(jnp.bfloat16))


def dot3(left, right, dims):
    def product(a, b):
        return lax.dot_general(a, b, dims, preferred_element_type=jnp.float32)

    if dims == TN:
        cross = product(left[0], right[1]) + product(left[1], right[0])
        return product(left[0], right[0]) + cross
    rows = left[0].shape[0]
    stacked = product(jnp.concatenate(left, axis=0), right[0])
    return stacked[:rows] + (stacked[rows:] + product(left[0], right[1]))


def spline_values(t):
    rest = 1.0 - t
    square = t * t
    cube = square * t
    return (
        rest * rest * rest / 6.0,
        (3.0 * cube - 6.0 * square + 4.0) / 6.0,
        (-3.0 * cube + 3.0 * square + 3.0 * t + 1.0) / 6.0,
        cube / 6.0,
    )


def spline_slopes(t):
    rest = 1.0 - t
    square = t * t
    return (-0.5 * rest * rest, 1.5 * square - 2.0 * t, -1.5 * square + t + 0.5, 0.5 * square)


def pick(masks, weights):
    chosen = jnp.where(masks[3], weights[3], 0.0)
    for step in (2, 1, 0):
        chosen = jnp.where(masks[step], weights[step], chosen)
    return chosen


def masks_of(slots, start):
    steps = slots - start
    return [steps == step for step in range(4)]


def rows_iota(rows, width):
    return lax.broadcasted_iota(jnp.int32, (rows, width), 0)


class Stencil:
    def __init__(self, cells, offs, span):
        self.near_x = cells[0, :, span] - lax.axis_index("px") * CX
        self.near_y = cells[1, :, span] - lax.axis_index("py") * CY
        self.near_z = cells[2, :, span]
        self.width = self.near_x.shape[1]
        self.t = [offs[d, :, span] for d in range(3)]

    def x(self):
        return masks_of(rows_iota(24, self.width), self.near_x)

    def y(self):
        return masks_of(rows_iota(CY, self.width), self.near_y)

    def rim(self):
        rim = rows_iota(ROWS - MAIN, self.width)
        return masks_of(rim // RIM, self.near_x), masks_of(CY + rim % RIM, self.near_y)

    def z(self):
        steps = (rows_iota(NZ, self.width) - self.near_z) & (NZ - 1)
        return [steps == step for step in range(4)]

    def values(self, d):
        return spline_values(self.t[d])

    def slopes(self, d):
        return spline_slopes(self.t[d])


class Exchange:
    def __init__(self, pieces_x, src, dst, lanes, send_sem, recv_sem):
        self.pieces_x, self.src, self.dst, self.lanes = pieces_x, src, dst, lanes
        self.send_sem, self.recv_sem = send_sem, recv_sem
        self.pieces = src.shape[0]
        self.mine = lax.axis_index("py") * pieces_x + lax.axis_index("px")

    def copy(self, step, here, there):
        peer = (self.mine + step) % self.pieces
        return pltpu.make_async_remote_copy(
            src_ref=self.src.at[peer if here is None else here, :, self.lanes],
            dst_ref=self.dst.at[there, :, self.lanes],
            send_sem=self.send_sem,
            recv_sem=self.recv_sem,
            device_id=(peer % self.pieces_x, peer // self.pieces_x),
            device_id_type=pl.DeviceIdType.MESH,
        )

    def put(self, value):
        self.src[:, :, self.lanes] = value.reshape(self.src.shape[:2] + (value.shape[1],))

        for step in range(1, self.pieces):
            self.copy(step, None, self.mine).start()

        self.dst[self.mine, :, self.lanes] = self.src[self.mine, :, self.lanes]

    def get(self):
        every = pl.ds(0, self.pieces - 1)
        self.copy(1, every, every).wait()
        return self.dst[:, :, self.lanes].reshape(NZ, -1)


def kernel(
    pieces_x, pieces_y, cells, offs, charge, spacing, beta, tz_h, tz_l, ty_h, ty_l, mx_hbm_h,
    mx_hbm_l, row1, row3, rowm, col2, colm, forces, energy, grid, wide, mx_h, mx_l, rz_h, rz_l,
    dz_h, dz_l, window, part, weight, src, dst, back, home, table_sem, send_sem, recv_sem,
):
    pieces = pieces_x * pieces_y
    slice_z = NZ // pieces
    mine = lax.axis_index("py") * pieces_x + lax.axis_index("px")
    core, edge = pl.ds(0, CORE), pl.ds(CORE, ROWS - CORE)
    loads = [
        pltpu.make_async_copy(mx_hbm_h, mx_h, table_sem.at[0]),
        pltpu.make_async_copy(mx_hbm_l, mx_l, table_sem.at[1]),
    ]
    for load in loads:
        load.start()
    barrier = pltpu.get_barrier_semaphore()

    for step in range(1, pieces):
        peer = (mine + step) % pieces
        pl.semaphore_signal(
            barrier,
            inc=1,
            device_id=(peer % pieces_x, peer // pieces_x),
            device_id_type=pl.DeviceIdType.MESH,
        )

    def tiles(body):
        @pl.loop(0, charge.shape[1] // (TILE * TWIN))
        def _(step):
            for twin in range(TWIN):
                span = pl.ds(pl.multiple_of((step * TWIN + twin) * TILE, TILE), TILE)
                body(span, Stencil(cells, offs, span), charge[:, span])

    tz = (tz_h[...], tz_l[...])
    grid[...] = jnp.zeros_like(grid)

    def spread_core(span, near, amount):
        row_x = pick(near.x(), [w * amount for w in near.values(0)])
        row_y = pick(near.y(), near.values(1))
        planes = jnp.concatenate([row_x[x : x + 1] * row_y for x in range(CX)], axis=0)
        profile = halves(pick(near.z(), near.values(2)))
        rz_h[:, span], rz_l[:, span] = profile
        grid[core, :] += dot3(halves(planes), profile, NT)

    tiles(spread_core)
    ahead = [
        Exchange(pieces_x, src, dst, lanes, send_sem.at[k], recv_sem.at[k])
        for k, lanes in enumerate((core, edge))
    ]
    value = dot3(tz, halves(grid[core, :]), NT)
    pl.semaphore_wait(barrier, pieces - 1)
    ahead[0].put(value)

    def spread_edge(span, near, amount):
        heavy = [w * amount for w in near.values(0)]
        row_x = pick(near.x(), heavy)
        row_y = pick(near.y(), near.values(1))
        rim_x, rim_y = near.rim()
        rim = pick(rim_x, heavy) * pick(rim_y, near.values(1))
        planes = [row_x[x : x + 1] * row_y for x in range(CX, SPAN)] + [rim]
        planes = jnp.concatenate(planes, axis=0)
        grid[edge, :] += dot3(halves(planes), (rz_h[:, span], rz_l[:, span]), NT)

    tiles(spread_edge)
    ahead[1].put(dot3(tz, halves(grid[edge, :]), NT))

    def slopes_z(span, near, amount):
        dz_h[:, span], dz_l[:, span] = halves(pick(near.z(), near.slopes(2)))

    tiles(slopes_z)

    chunk = pieces_x * slice_z
    total_x = CX * pieces_x
    total_y = CY * pieces_y
    split = CX * chunk
    turned = grid

    def main_corners(planes):
        for x in planes:
            for j in range(pieces_y):
                lanes, own = pl.ds(x * chunk, chunk), pl.ds(j * chunk, chunk)
                yield (pl.ds(x * CY, CY), own), (pl.ds(j * CY, CY), lanes)

    def rim_corners():
        for x in range(SPAN):
            for j in range(pieces_y):
                lanes, own = pl.ds(x * chunk, chunk), pl.ds(j * chunk, chunk)
                yield (pl.ds(MAIN + x * RIM, RIM), own), (pl.ds(total_y + j * RIM, RIM), lanes)

    def edge_corners():
        yield from main_corners(range(CX, SPAN))
        yield from rim_corners()

    tails = pl.ds(split, wide.shape[1] - split)
    wide[:, tails] = jnp.zeros((wide.shape[0], wide.shape[1] - split), jnp.float32)
    ty = (ty_h[:, :total_y], ty_l[:, :total_y])
    ty_rim = (ty_h[:, total_y:], ty_l[:, total_y:])
    width = mx_h.shape[1]

    def spread_scalar(ref, place):
        return jnp.full((1, width), ref[place], jnp.float32)

    s0, s1, s2 = (spread_scalar(spacing, d) for d in range(3))
    b = spread_scalar(beta, 0)
    squares = row1[...] / (s0 * s0) + row3[pl.ds(mine, 1), :] / (s2 * s2)
    squares = squares + col2[...] * (1.0 / (s1 * s1))
    safe = jnp.where(squares > 0.0, squares, 1.0)
    volume = s0 * s1 * s2 * float(total_x * total_y * NZ)
    table = jnp.exp(safe * (-(np.pi**2) / (b * b))) / (safe * (np.pi * volume))
    table = table * (rowm[pl.ds(mine, 1), :] * colm[...])
    weight[...] = jnp.where(squares > 0.0, table, 0.0)
    for load in loads:
        load.wait()
    turned[core, :] = ahead[0].get().T
    for narrow, broad in main_corners(range(CX)):
        wide[broad] = turned[narrow]
    first = dot3(ty, halves(wide[:total_y, :split]), NN)
    turned[edge, :] = ahead[1].get().T
    for narrow, broad in edge_corners():
        wide[broad] = turned[narrow]
    last = dot3(ty, halves(wide[:total_y, split:]), NN)
    mixed = jnp.concatenate([first, last], axis=1) + dot3(ty_rim, halves(wide[total_y:, :]), NN)
    mx = (mx_h[...], mx_l[...])
    spectrum = dot3(halves(mixed), mx, NN)
    spectrum = spectrum * weight[...]
    mixed = halves(dot3(halves(spectrum), mx, NT))
    after = [
        Exchange(pieces_x, back, home, lanes, send_sem.at[2 + k], recv_sem.at[2 + k])
        for k, lanes in enumerate((core, edge))
    ]
    wide[total_y:, :] = dot3(ty_rim, mixed, TN)
    wide[:total_y, split:] = dot3(ty, tuple(half[:, split:] for half in mixed), TN)
    turned[edge, :] = jnp.zeros((ROWS - CORE, NZ), jnp.float32)
    for narrow, broad in edge_corners():
        turned[narrow] = wide[broad]
    after[1].put(turned[edge, :].T)
    wide[:total_y, :split] = dot3(ty, tuple(half[:, :split] for half in mixed), TN)
    for narrow, broad in main_corners(range(CX)):
        turned[narrow] = wide[broad]
    after[0].put(turned[core, :].T)

    def fields(rows, span):
        def sampled_with(high, low):
            stacked = jnp.dot(
                window[: 2 * rows], high[:, span], preferred_element_type=jnp.float32
            )
            rest = jnp.dot(window[:rows], low[:, span], preferred_element_type=jnp.float32)
            return stacked[:rows] + (stacked[rows:] + rest)

        return sampled_with(rz_h, rz_l), sampled_with(dz_h, dz_l)

    def over_x(planes, rows, field):
        total = rows[planes[0] : planes[0] + 1] * field[0:CY]
        for k, x in enumerate(planes[1:], 1):
            total = total + rows[x : x + 1] * field[k * CY : (k + 1) * CY]
        return total

    def four_sums(planes, near, level, tilt):
        masks_x, masks_y = near.x(), near.y()
        row_x, tilt_x = pick(masks_x, near.values(0)), pick(masks_x, near.slopes(0))
        row_y, tilt_y = pick(masks_y, near.values(1)), pick(masks_y, near.slopes(1))
        plain = over_x(planes, row_x, level)
        return [
            jnp.sum(product, axis=0, keepdims=True)
            for product in (
                over_x(planes, tilt_x, level) * row_y,
                plain * tilt_y,
                over_x(planes, row_x, tilt) * row_y,
                plain * row_y,
            )
        ]

    def set_window(got):
        field = halves(dot3(halves(got.T), tz, NN))
        window[: 2 * got.shape[1]] = jnp.concatenate(field, axis=0)

    def gather_edge(span, near, amount):
        level, tilt = fields(ROWS - CORE, span)
        sums = four_sums(range(CX, SPAN), near, level, tilt)
        masks_x, masks_y = near.rim()
        row_x, tilt_x = pick(masks_x, near.values(0)), pick(masks_x, near.slopes(0))
        row_y, tilt_y = pick(masks_y, near.values(1)), pick(masks_y, near.slopes(1))
        level, tilt = level[MAIN - CORE :], tilt[MAIN - CORE :]
        flat = row_x * row_y
        extra = (level * tilt_x * row_y, level * row_x * tilt_y, tilt * flat, level * flat)
        for d in range(4):
            part[d, :, span] = sums[d] + jnp.sum(extra[d], axis=0, keepdims=True)

    set_window(after[1].get())
    tiles(gather_edge)

    def gather_core(span, near, amount):
        sums = four_sums(range(CX), near, *fields(CORE, span))
        for d in range(3):
            scale = jnp.full((1, TILE), spacing[d], jnp.float32)
            forces[d, :, span] = -amount * (sums[d] + part[d, :, span]) / scale
        energy[:, span] = 0.5 * amount * (sums[3] + part[3, :, span])

    set_window(after[0].get())
    tiles(gather_core)


def signed(length):
    index = np.arange(length)
    return np.where(2 * index < length, index, index - length)


def moduli(length):
    return 1.0 / ((2.0 + np.cos(2.0 * np.pi / length * np.arange(length))) / 3.0) ** 2


def middle_tables(pieces_x, pieces_y):
    pieces = pieces_x * pieces_y
    slice_z = NZ // pieces
    total_x, total_y = CX * pieces_x, CY * pieces_y
    rim = np.zeros((total_y, pieces_y, RIM))
    starts = CY * (np.arange(pieces_y) + 1)
    places = starts[:, None] + np.arange(RIM - 1)[None, :]
    rim[:, :, : RIM - 1] = cas(places.reshape(-1), total_y).reshape(total_y, pieces_y, RIM - 1)
    ty = np.concatenate([cas(np.arange(total_y), total_y), rim.reshape(total_y, -1)], axis=1)
    places = (np.arange(SPAN)[:, None] + CX * np.arange(pieces_x)[None, :]).reshape(-1)
    mx = np.kron(cas(places, total_x).T, np.eye(slice_z))
    depth = -(-mx.shape[0] // 128) * 128
    mx = np.concatenate([mx, np.zeros((depth - mx.shape[0], mx.shape[1]))], axis=0)
    row1 = np.repeat((signed(total_x) / total_x) ** 2, slice_z)[None, :]
    row3 = np.tile(((signed(NZ) / NZ) ** 2).reshape(pieces, slice_z), (1, total_x))
    rowm = np.tile(moduli(NZ).reshape(pieces, slice_z), (1, total_x))
    rowm = rowm * np.repeat(moduli(total_x), slice_z)[None, :]
    col2 = ((signed(total_y) / total_y) ** 2)[:, None]
    colm = moduli(total_y)[:, None]
    plain = tuple(jnp.asarray(t, jnp.float32) for t in (row1, row3, rowm, col2, colm))
    return constant_halves(ty) + constant_halves(mx) + plain


def local(base_cell, cell_offset, charges, spacing, ewald_beta):
    pieces_x = lax.axis_size("px")
    pieces_y = lax.axis_size("py")
    pieces = pieces_x * pieces_y
    charge = charges.reshape(1, -1)
    atoms = charge.shape[1]
    cells = jnp.transpose(base_cell, (0, 3, 1, 2)).reshape(3, 1, atoms)
    offs = jnp.transpose(cell_offset, (0, 3, 1, 2)).reshape(3, 1, atoms)
    tz = constant_halves(cas(np.arange(NZ), NZ))
    tables = middle_tables(pieces_x, pieces_y)
    vmem = pl.BlockSpec(memory_space=pltpu.VMEM)
    scalars = pl.BlockSpec(memory_space=pltpu.SMEM)
    anywhere = pl.BlockSpec(memory_space=pl.ANY)
    blocks = pltpu.VMEM((pieces, NZ // pieces, ROWS), jnp.float32)
    profile = pltpu.VMEM((NZ, atoms), jnp.bfloat16)
    forces, energy = pl.pallas_call(
        functools.partial(kernel, pieces_x, pieces_y),
        out_shape=(
            jax.ShapeDtypeStruct((3, 1, atoms), jnp.float32),
            jax.ShapeDtypeStruct((1, atoms), jnp.float32),
        ),
        in_specs=[vmem] * 3 + [scalars] * 2 + [vmem] * 4 + [anywhere] * 2 + [vmem] * 5,
        out_specs=(vmem, vmem),
        scratch_shapes=[
            pltpu.VMEM((ROWS, NZ), jnp.float32),
            pltpu.VMEM((tables[0].shape[1], tables[2].shape[0]), jnp.float32),
            pltpu.VMEM(tables[2].shape, jnp.bfloat16),
            pltpu.VMEM(tables[2].shape, jnp.bfloat16),
            profile,
            profile,
            profile,
            profile,
            pltpu.VMEM((2 * CORE, NZ), jnp.bfloat16),
            pltpu.VMEM((4, 1, atoms), jnp.float32),
            pltpu.VMEM((tables[0].shape[0], tables[2].shape[1]), jnp.float32),
            blocks,
            blocks,
            blocks,
            blocks,
            pltpu.SemaphoreType.DMA((2,)),
            pltpu.SemaphoreType.DMA((4,)),
            pltpu.SemaphoreType.DMA((4,)),
        ],
        compiler_params=pltpu.CompilerParams(
            vmem_limit_bytes=VMEM_LIMIT, collective_id=0, has_side_effects=True
        ),
        name="ewald",
    )(cells, offs, charge, spacing, ewald_beta, *tz, *tables)
    forces = jnp.transpose(forces.reshape(1, 3, 1, atoms), (0, 2, 3, 1))
    return forces, energy.reshape(charges.shape)


def solution(mesh):
    placed = (P("px", "py", None, None), P("px", "py", None, None), P("px", "py", None), P(), P())
    return jax.shard_map(
        local,
        mesh=mesh,
        in_specs=placed,
        out_specs=(P("px", "py", None, None), P("px", "py", None)),
        check_vma=False,
    )
```
